32 devices in a mesh: dp: 1 (over z), pp: 4 (over y), tp: 8 (over x, core).
Axes of the slice: x: 4, y: 4, z: 1, core: 2. Of those that a mesh axis runs over, the one named last changes fastest.
The devices are a block of a 4x4x8 slice.
Arguments:
- x_in: bfloat16 [16, 64, 3072], P('dp', 'tp')
- ln_gain: bfloat16 [2, 4, 3072], P(None, 'pp')
- w_in: bfloat16 [2, 4, 3072, 8192], P(None, 'pp', None, 'tp')
- w_out: bfloat16 [2, 4, 8192, 3072], P(None, 'pp', 'tp')
Outputs:
- output: bfloat16 [16, 64, 3072], P(('dp', 'pp'), 'tp')
All inputs are finite; a program needn't handle non-finite values.
Results may differ from the reference program's by a relative error of at most 0.02.
Values are sent between devices in bfloat16 or wider.
A program may use at most 768 MiB of HBM per device.

```python
import jax
import jax.numpy as jnp
from jax import lax

MODEL_DIM = 3072
FFN_DIM = 8192
STAGES = 4
TP_RANKS = 8
MICRO_BATCHES = 16
SEQ_TOKENS = 64

NORM_EPS = 1e-5
SHARD_FFN = FFN_DIM // TP_RANKS
BLOCK_COUNT = 2 * STAGES


def setup_inputs(seed: int = 0, part: int = 0) -> dict:
    base_key = jax.random.key(seed)
    act_key = jax.random.fold_in(jax.random.fold_in(base_key, 1), part)
    gain_key, first_key, second_key = jax.random.split(jax.random.fold_in(base_key, 2), 3)
    x_vals = jax.random.normal(act_key, (MICRO_BATCHES, SEQ_TOKENS, MODEL_DIM), jnp.float32)
    gain_vals = 1.0 + 0.25 * jax.random.normal(gain_key, (2, STAGES, MODEL_DIM), jnp.float32)
    first_vals = jax.random.normal(first_key, (2, STAGES, MODEL_DIM, FFN_DIM), jnp.float32) * MODEL_DIM ** -0.5
    second_vals = jax.random.normal(second_key, (2, STAGES, FFN_DIM, MODEL_DIM), jnp.float32) * FFN_DIM ** -0.5
    return {"x_in": x_vals.astype(jnp.bfloat16), "ln_gain": gain_vals.astype(jnp.bfloat16), "w_in": first_vals.astype(jnp.bfloat16), "w_out": second_vals.astype(jnp.bfloat16)}


def mlp_block(resid, gain_vec, w_first, w_second):
    resid_f = resid.astype(jnp.float32)
    row_mean = jnp.mean(resid_f, axis=-1, keepdims=True)
    centred = resid_f - row_mean
    row_var = jnp.mean(centred * centred, axis=-1, keepdims=True)
    normed = (centred * lax.rsqrt(row_var + NORM_EPS) * gain_vec.astype(jnp.float32)).astype(jnp.bfloat16)
    hidden = jax.nn.gelu(jnp.dot(normed, w_first, preferred_element_type=jnp.float32)).astype(jnp.bfloat16)
    hidden_shards = hidden.reshape(SEQ_TOKENS, TP_RANKS, SHARD_FFN).transpose(1, 0, 2)
    w_shards = w_second.reshape(TP_RANKS, SHARD_FFN, MODEL_DIM)

    def add_shard(acc_sum, shard_pair):
        h_shard, w_shard = shard_pair
        part_prod = jnp.dot(h_shard, w_shard, preferred_element_type=jnp.float32)
        return acc_sum + part_prod.astype(jnp.bfloat16).astype(jnp.float32), None

    mlp_sum, _ = lax.scan(add_shard, jnp.zeros((SEQ_TOKENS, MODEL_DIM), jnp.float32), (hidden_shards, w_shards))
    return (resid_f + mlp_sum).astype(jnp.bfloat16)


def reference(x_in, ln_gain, w_in, w_out):
    gain_rows = ln_gain.reshape(BLOCK_COUNT, MODEL_DIM)
    firsts = w_in.reshape(BLOCK_COUNT, MODEL_DIM, FFN_DIM)
    seconds = w_out.reshape(BLOCK_COUNT, FFN_DIM, MODEL_DIM)

    def one_block(resid, block_w):
        gain_vec, w_first, w_second = block_w
        return mlp_block(resid, gain_vec, w_first, w_second), None

    def one_micro(micro_x):
        result, _ = lax.scan(one_block, micro_x, (gain_rows, firsts, seconds))
        return result

    return lax.map(one_micro, x_in)
```

```python
import functools

import jax
import jax.numpy as jnp
from jax import lax
from jax.experimental import pallas as pl
from jax.experimental.pallas import tpu as pltpu
from jax.sharding import PartitionSpec as P

MESH = pl.DeviceIdType.MESH
NORM_EPS = 1e-5
CORES = 2
LOOKAHEAD = 2


def _f32(a):
    return a.astype(jnp.float32)


def _bf16(a):
    return a.astype(jnp.bfloat16)


def _kernel(dims, x_hbm, gain_ref, w1_hbm, w2_hbm, out_ref,
            w1, w2, xs, xbuf, ybuf, rbuf, hbuf, abuf, sbuf, fbuf, obuf,
            wl_sem, wp_send, wp_recv, xl_sem, x_send, x_recv,
            rs_send, rs_recv, ag_send, ag_recv, f_send, f_recv):
    stages, chips, visits, tok, width, hid = dims
    ranks = chips * CORES
    slab = width // chips
    tsh = tok // ranks
    p = lax.axis_index("pp")
    t = lax.axis_index("tp")
    c = t // CORES
    k = lax.rem(t, CORES)
    nxt = lax.rem(p + 1, stages)
    at_start = p == 0
    at_end = p == stages - 1

    def dev(pp, chip, core):
        return {"pp": pp, "tp": chip * CORES + core}

    def remote(src, dst, ssem, rsem, where):
        return pltpu.make_async_remote_copy(src_ref=src, dst_ref=dst, send_sem=ssem, recv_sem=rsem,
                                            device_id=where, device_id_type=MESH)

    def local_wait(ref, sem):
        pltpu.make_async_copy(ref, ref, sem).wait()

    def load_w(v):
        return (pltpu.make_async_copy(w1_hbm.at[v], w1.at[v, k], wl_sem.at[v, 0]),
                pltpu.make_async_copy(w2_hbm.at[v], w2.at[v, k], wl_sem.at[v, 1]))

    def push_w(v):
        other = dev(p, c, 1 - k)
        return (remote(w1_hbm.at[v], w1.at[v, k], wp_send.at[v, 0], wp_recv.at[v, 0], other),
                remote(w2_hbm.at[v], w2.at[v, k], wp_send.at[v, 1], wp_recv.at[v, 1], other))

    x_load = pltpu.make_async_copy(x_hbm, xs, xl_sem)
    x_load.start()
    for v in range(2):
        for cp in load_w(v):
            cp.start()

    bar = pltpu.get_barrier_semaphore()
    for pp in range(stages):
        for tt in range(ranks):
            @pl.when((pp != p) | (tt != t))
            def _(pp=pp, tt=tt):
                pl.semaphore_signal(bar, inc=1, device_id={"pp": pp, "tp": tt}, device_id_type=MESH)
    pl.semaphore_wait(bar, stages * ranks - 1)
    x_load.wait()

    def x_copy(i, core, chip):
        return remote(xs.at[CORES * i + core], xbuf.at[i, t], x_send.at[chip], x_recv.at[i, t], dev(p, chip, core))

    def x_share(i):
        xbuf[i, t] = xs[CORES * i + k]
        for d in range(1, chips):
            for dk in range(CORES):
                x_copy(i, lax.rem(k + dk, CORES), lax.rem(c + d, chips)).start()

    @pl.when(at_start)
    def _():
        for i in range(visits):
            x_copy(i, 1 - k, c).start()
        for i in range(LOOKAHEAD):
            x_share(i)

    for v in range(2):
        for cp in push_w(v):
            cp.start()

    def visit(idx, carry):
        v = idx // visits
        i = lax.rem(idx, visits)
        par = lax.rem(idx, 2)
        first = at_start & (v == 0)
        last = at_end & (v == 1)

        @pl.when(first & (i + LOOKAHEAD < visits))
        def _():
            x_share(i + LOOKAHEAD)

        @pl.when(first)
        def _():
            for r in range(ranks):
                @pl.when(r != t)
                def _(r=r):
                    local_wait(xbuf.at[i, r], x_recv.at[i, r])
            for q in range(chips):
                ybuf[i, q] = _bf16(_f32(xbuf[i, :, :, q * slab:(q + 1) * slab]).reshape(tok, slab))

        def ag_copy(d):
            return remote(ybuf.at[i, c], ybuf.at[i, c], ag_send.at[par, d - 1], ag_recv.at[i, c],
                          dev(p, lax.rem(c + d, chips), k))

        @pl.when(jnp.logical_not(first))
        def _():
            for q in range(chips):
                local_wait(rbuf.at[i, q], rs_recv.at[i, q])
            total = _f32(rbuf[i, 0])
            for q in range(1, chips):
                total = total + _f32(rbuf[i, q])
            ybuf[i, c] = _bf16(total)
            for d in (2, 1, 3):
                ag_copy(d).start()
            for d in range(1, chips):
                q = lax.rem(c + d, chips)
                local_wait(ybuf.at[i, q], ag_recv.at[i, q])
            for d in range(1, chips):
                ag_copy(d).wait_send()

        part = [_f32(ybuf[i, q]) for q in range(chips)]
        mean = sum(jnp.sum(a, axis=-1, keepdims=True) for a in part) * (1.0 / width)
        var = jnp.zeros_like(mean)
        for q in range(chips):
            a = _f32(ybuf[i, q]) - mean
            var = var + jnp.sum(a * a, axis=-1, keepdims=True)
        scale = lax.rsqrt(var * (1.0 / width) + NORM_EPS)
        for q in range(chips):
            cols = slice(q * slab, (q + 1) * slab)
            hbuf[:, cols] = _bf16((_f32(ybuf[i, q]) - mean) * scale * _f32(gain_ref[v, :, cols]))

        def wait_weights(j):
            @pl.when(i == 0)
            def _():
                load_w(v)[j].wait()
                push_w(v)[j].wait_recv()

        wait_weights(0)
        for s in range(CORES):
            for n in range(0, hid, 512):
                acc = jnp.dot(hbuf[...], w1[v, s, :, n:n + 512], preferred_element_type=jnp.float32)
                abuf[s, :, n:n + 512] = _bf16(jax.nn.gelu(acc))
        wait_weights(1)

        def rs_copy(d):
            return remote(sbuf.at[par, d], rbuf.at[i, c], rs_send.at[par, d], rs_recv.at[i, c],
                          dev(nxt, lax.rem(c + d, chips), k))

        for d in (2, 1, 3, 0):
            q = lax.rem(c + d, chips)
            cols = pl.ds(pl.multiple_of(q * slab, slab), slab)
            prod = jnp.zeros((tok, slab), jnp.float32)
            for s in range(CORES):
                prod = prod + _f32(_bf16(jnp.dot(abuf[s], w2[v, s, :, cols], preferred_element_type=jnp.float32)))

            @pl.when(jnp.logical_not(last))
            def _():
                @pl.when(idx >= 2)
                def _():
                    rs_copy(d).wait_send()
                if d == 0:
                    sbuf[par, d] = _bf16(prod + _f32(ybuf[i, c]))
                else:
                    sbuf[par, d] = _bf16(prod)
                rs_copy(d).start()

            @pl.when(last)
            def _():
                row_chip = lax.broadcasted_iota(jnp.int32, (tok, slab), 0) // (tsh * CORES)
                resid = jnp.where(row_chip == c, _f32(ybuf[i, q]), 0.0)
                fbuf[:, :, cols] = _bf16((prod + resid).reshape(ranks, tsh, slab))

        @pl.when(last)
        def _():
            dst_stage = (CORES * i) // (visits * CORES // stages)
            slot = lax.rem(CORES * i, visits * CORES // stages) + k

            def f_copy(r):
                return remote(fbuf.at[r], obuf.at[slot, c], f_send.at[r], f_recv.at[slot, c], {"pp": dst_stage, "tp": r})

            for r in range(ranks):
                mine = (dst_stage == p) & (r == t)

                @pl.when(mine)
                def _(r=r):
                    obuf[slot, c] = fbuf[r]

                @pl.when(jnp.logical_not(mine))
                def _(r=r):
                    f_copy(r).start()
            for r in range(ranks):
                @pl.when((dst_stage != p) | (r != t))
                def _(r=r):
                    f_copy(r).wait_send()
        return carry

    lax.fori_loop(0, 2 * visits, visit, 0)

    per_stage = visits * CORES // stages
    for j in range(per_stage):
        for q in range(chips):
            mine = at_end & (q == c) & (k == j % CORES)

            @pl.when(jnp.logical_not(mine))
            def _(j=j, q=q):
                local_wait(obuf.at[j, q], f_recv.at[j, q])
        total = _f32(obuf[j, 0])
        for q in range(1, chips):
            total = total + _f32(obuf[j, q])
        out_ref[j] = _bf16(total)

    for par in range(2):
        for d in range(chips):
            local_wait(sbuf.at[par, d], rs_send.at[par, d])
    for v in range(2):
        for cp in push_w(v):
            cp.wait_send()

    @pl.when(at_start)
    def _():
        for d in range(chips):
            chip = lax.rem(c + d, chips)
            ref = xs.at[pl.ds(0, visits)] if d == 0 else xs
            local_wait(ref, x_send.at[chip])


def solution(mesh):
    stages, ranks = mesh.shape["pp"], mesh.shape["tp"]
    chips = ranks // CORES

    def per_device(x, gain, w_in, w_out):
        micro, tsh, width = x.shape
        passes, _, _, hid = w_in.shape
        tok = tsh * ranks
        visits = micro // CORES
        slab = width // chips
        per_stage = micro // stages
        dims = (stages, chips, visits, tok, width, hid)
        bf = jnp.bfloat16
        dma = pltpu.SemaphoreType.DMA
        any_space = pl.BlockSpec(memory_space=pl.ANY)
        vmem = pl.BlockSpec(memory_space=pltpu.VMEM)
        return pl.pallas_call(
            functools.partial(_kernel, dims),
            name="mlp_pipe",
            out_shape=jax.ShapeDtypeStruct((per_stage, tsh, width), bf),
            in_specs=[any_space, vmem, any_space, any_space],
            out_specs=vmem,
            scratch_shapes=[
                pltpu.VMEM((passes, CORES, width, hid), bf),
                pltpu.VMEM((passes, CORES, hid, width), bf),
                pltpu.VMEM((micro, tsh, width), bf),
                pltpu.VMEM((visits, ranks, tsh, width), bf),
                pltpu.VMEM((visits, chips, tok, slab), bf),
                pltpu.VMEM((visits, chips, tok, slab), bf),
                pltpu.VMEM((tok, width), bf),
                pltpu.VMEM((CORES, tok, hid), bf),
                pltpu.VMEM((2, chips, tok, slab), bf),
                pltpu.VMEM((ranks, tsh, width), bf),
                pltpu.VMEM((per_stage, chips, tsh, width), bf),
                dma((passes, 2)), dma((passes, 2)), dma((passes, 2)),
                dma, dma((chips,)), dma((visits, ranks)),
                dma((2, chips)), dma((visits, chips)), dma((2, chips - 1)), dma((visits, chips)),
                dma((ranks,)), dma((per_stage, chips)),
            ],
            compiler_params=pltpu.CompilerParams(collective_id=0, has_side_effects=True, vmem_limit_bytes=67043328),
        )(x, gain, w_in.reshape(passes, width, hid), w_out.reshape(passes, hid, width))

    return jax.shard_map(
        per_device,
        mesh=mesh,
        in_specs=(P("dp", "tp", None), P(None, "pp", None), P(None, "pp", None, "tp"), P(None, "pp", "tp", None)),
        out_specs=P(("dp", "pp"), "tp", None),
        check_vma=False,
    )
```

```python
import functools

import jax
import jax.numpy as jnp
from jax import lax
from jax.experimental import pallas as pl
from jax.experimental.pallas import tpu as pltpu
from jax.sharding import PartitionSpec as P

MESH = pl.DeviceIdType.MESH
NORM_EPS = 1e-5
CORES = 2
LOOKAHEAD = 2
REDUCE_AT = 2
FORWARD_AT = 5


def _f32(a):
    return a.astype(jnp.float32)


def _bf16(a):
    return a.astype(jnp.bfloat16)


def _kernel(dims, x_hbm, gain_ref, w1_hbm, w2_hbm, out_ref,
            w1, w2, xs, xbuf, ybuf, rbuf, lbuf, hold, hbuf, abuf, sbuf, fbuf, obuf,
            wl_sem, wp_send, wp_recv, xl_sem, x_send, x_recv, ready,
            rs_send, rs_recv, l_recv, ag_send, ag_first, ag_rest, f_send, f_recv):
    stages, chips, visits, tok, width, hid = dims
    ranks = chips * CORES
    slab = width // chips
    half = slab // 2
    tsh = tok // ranks
    per_stage = visits * CORES // stages
    p = lax.axis_index("pp")
    t = lax.axis_index("tp")
    c = t // CORES
    k = lax.rem(t, CORES)
    nxt = lax.rem(p + 1, stages)
    right, left = lax.rem(c + 1, chips), lax.rem(c + chips - 1, chips)
    far = lax.rem(c + 2, chips)
    at_start = p == 0
    at_end = p == stages - 1

    def dev(pp, chip, core):
        return {"pp": pp, "tp": chip * CORES + core}

    def remote(src, dst, ssem, rsem, where):
        return pltpu.make_async_remote_copy(src_ref=src, dst_ref=dst, send_sem=ssem, recv_sem=rsem,
                                            device_id=where, device_id_type=MESH)

    def wait(ref, sem):
        pltpu.make_async_copy(ref, ref, sem).wait()

    def load_w(v, j):
        src, dst = ((w1_hbm, w1), (w2_hbm, w2))[j]
        return pltpu.make_async_copy(src.at[v], dst.at[v, k], wl_sem.at[v, j])

    def push_w(v, j):
        src, dst = ((w1_hbm, w1), (w2_hbm, w2))[j]
        return remote(src.at[v], dst.at[v, k], wp_send.at[v, j], wp_recv.at[v, j], dev(p, c, 1 - k))

    x_load = pltpu.make_async_copy(x_hbm, xs, xl_sem)
    x_load.start()
    for v in range(2):
        for j in range(2):
            load_w(v, j).start()

    bar = pltpu.get_barrier_semaphore()
    for r in range(ranks):
        @pl.when(r != t)
        def _(r=r):
            pl.semaphore_signal(bar, inc=1, device_id={"pp": p, "tp": r}, device_id_type=MESH)

    @pl.when(jnp.logical_not(at_end))
    def _():
        for q in range(chips):
            pl.semaphore_signal(bar, inc=1, device_id=dev(nxt, q, k), device_id_type=MESH)
    pl.semaphore_wait(bar, jnp.where(at_start, ranks - 1, ranks - 1 + chips))

    @pl.when(jnp.logical_not(at_start))
    def _():
        for q in range(chips):
            pl.semaphore_signal(ready, inc=1, device_id=dev(p - 1, q, k), device_id_type=MESH)

    def x_copy(i, core, chip):
        return remote(xs.at[CORES * i + core], xbuf.at[i, t], x_send.at[chip], x_recv.at[i], dev(p, chip, core))

    def x_share(i):
        xbuf[i, t] = xs[CORES * i + k]
        for core in range(CORES):
            for chip in (far, right, left):
                x_copy(i, core, chip).start()

    @pl.when(at_start)
    def _():
        x_load.wait()
        for i in range(visits):
            x_copy(i, 1 - k, c).start()
        for i in range(LOOKAHEAD):
            x_share(i)

    for v in range(2):
        for j in range(2):
            push_w(v, j).start()

    def share(i, par, piece, chip, sem):
        return remote(ybuf.at[i, piece[0], piece[1]], ybuf.at[i, piece[0], piece[1]], ag_send.at[par], sem, dev(p, chip, k))

    def reduce_slab(idx):
        i = lax.rem(idx, visits)
        par = lax.rem(idx, 2)

        @pl.when(idx >= jnp.where(at_start, visits + 2, 2))
        def _():
            wait(ybuf.at[i, 0:3], ag_send.at[par])

        with jax.named_scope("wait_rs"):
            wait(rbuf.at[i], rs_recv.at[i])
        for h in range(2):
            ybuf[i, c, h] = _bf16(_f32(rbuf[i, 0, h]) + _f32(rbuf[i, 1, h]) + _f32(rbuf[i, 2, h]))
        share(i, par, (c, 0), right, ag_first.at[i, 0]).start()
        share(i, par, (c, 1), left, ag_first.at[i, 1]).start()
        share(i, par, (c, 1), right, ag_rest.at[i]).start()
        share(i, par, (c, 0), left, ag_rest.at[i]).start()

    def forward(idx):
        i = lax.rem(idx, visits)
        par = lax.rem(idx, 2)
        with jax.named_scope("wait_fwd"):
            wait(ybuf.at[i, left, 0], ag_first.at[i, 0])
        share(i, par, (left, 0), right, ag_rest.at[i]).start()
        with jax.named_scope("wait_fwd2"):
            wait(ybuf.at[i, right, 1], ag_first.at[i, 1])
        share(i, par, (right, 1), left, ag_rest.at[i]).start()

    @pl.when(jnp.logical_not(at_start))
    def _():
        reduce_slab(0)
        forward(0)

    def f_wait(i):
        dst_stage = (CORES * i) // per_stage
        for r in range(ranks):
            @pl.when((dst_stage != p) | (r != t))
            def _(r=r):
                wait(fbuf.at[i % 2, r], f_send.at[i % 2, r])

    def visit(idx, carry):
        v = idx // visits
        i = lax.rem(idx, visits)
        par = lax.rem(idx, 2)
        first = at_start & (v == 0)
        last = at_end & (v == 1)
        ahead = (idx + 1 < 2 * visits) & (idx + 1 != visits) & ((idx + 1 > visits) | jnp.logical_not(at_start))

        def at(place):
            @pl.when(ahead)
            def _():
                if place == REDUCE_AT:
                    reduce_slab(idx + 1)
                if place == FORWARD_AT:
                    forward(idx + 1)

        @pl.when(first & (i + LOOKAHEAD < visits))
        def _():
            x_share(i + LOOKAHEAD)

        @pl.when(first)
        def _():
            with jax.named_scope("wait_x"):
                wait(xbuf.at[i, 0:ranks - 1], x_recv.at[i])
            for q in range(chips):
                for h in range(2):
                    lo = q * slab + h * half
                    ybuf[i, q, h] = _bf16(_f32(xbuf[i, :, :, lo:lo + half]).reshape(tok, half))

        @pl.when(jnp.logical_not(first))
        def _():
            with jax.named_scope("wait_ag"):
                wait(ybuf.at[i, 0:2], ag_rest.at[i])

        at(0)

        pieces = [(q, h) for q in range(chips) for h in range(2)]
        mean = sum(jnp.sum(_f32(ybuf[i, q, h]), axis=-1, keepdims=True) for q, h in pieces) * (1.0 / width)
        var = jnp.zeros_like(mean)
        for q, h in pieces:
            a = _f32(ybuf[i, q, h]) - mean
            var = var + jnp.sum(a * a, axis=-1, keepdims=True)
        scale = lax.rsqrt(var * (1.0 / width) + NORM_EPS)
        for q, h in pieces:
            cols = slice(q * slab + h * half, q * slab + (h + 1) * half)
            hbuf[:, cols] = _bf16((_f32(ybuf[i, q, h]) - mean) * scale * _f32(gain_ref[v, :, cols]))

        def wait_weights(j):
            @pl.when(i == 0)
            def _():
                load_w(v, j).wait()
                push_w(v, j).wait_recv()

        at(1)
        with jax.named_scope("wait_w1"):
            wait_weights(0)
        for s in range(CORES):
            for n in range(0, hid, 512):
                acc = jnp.dot(hbuf[...], w1[v, s, :, n:n + 512], preferred_element_type=jnp.float32)
                abuf[s, :, n:n + 512] = _bf16(jax.nn.gelu(acc))
            at(2 + s)
        with jax.named_scope("wait_w2"):
            wait_weights(1)

        @pl.when(idx == 0)
        def _():
            @pl.when(jnp.logical_not(at_end))
            def _():
                pl.semaphore_wait(ready, chips)

        @pl.when(jnp.logical_not(last) & (idx >= 2))
        def _():
            wait(sbuf.at[par], rs_send.at[par])

        @pl.when(last & (i >= 2))
        def _():
            f_wait(i - 2)

        def product(q):
            cols = pl.ds(pl.multiple_of(q * slab, slab), slab)
            prod = jnp.zeros((tok, slab), jnp.float32)
            for s in range(CORES):
                prod = prod + _f32(_bf16(jnp.dot(abuf[s], w2[v, s, :, cols], preferred_element_type=jnp.float32)))

            @pl.when(last)
            def _():
                row_chip = lax.broadcasted_iota(jnp.int32, (tok, slab), 0) // (tsh * CORES)
                whole = jnp.concatenate([_f32(ybuf[i, q, 0]), _f32(ybuf[i, q, 1])], axis=1)
                fbuf[par, :, :, cols] = _bf16((prod + jnp.where(row_chip == c, whole, 0.0)).reshape(ranks, tsh, slab))
            return prod[:, :half], prod[:, half:]

        def partial(slot, h, dst, where, sem):
            return remote(sbuf.at[par, slot, h], dst, rs_send.at[par], sem, where)

        going = jnp.logical_not(last)
        far_prod = product(far)

        @pl.when(going)
        def _():
            for h, chip in ((0, right), (1, left)):
                sbuf[par, 0, h] = _bf16(far_prod[h])
                partial(0, h, lbuf.at[par, h], dev(p, chip, k), l_recv.at[par, h]).start()
        at(4)

        for slot, chip, h in ((1, right, 1), (2, left, 0)):
            prod = product(chip)

            @pl.when(going)
            def _(slot=slot, chip=chip, h=h, prod=prod):
                sbuf[par, slot, h] = _bf16(prod[h])
                hold[1 - h] = prod[1 - h]
                partial(slot, h, rbuf.at[i, slot, h], dev(nxt, chip, k), rs_recv.at[i]).start()
            at(4 + slot)

        own_prod = product(c)

        @pl.when(going)
        def _():
            for h in range(2):
                sbuf[par, 3, h] = _bf16(own_prod[h] + _f32(ybuf[i, c, h]))
            remote(sbuf.at[par, 3], rbuf.at[i, 0], rs_send.at[par], rs_recv.at[i], dev(nxt, c, k)).start()
        at(7)

        @pl.when(going)
        def _():
            for slot, chip, h in ((1, right, 0), (2, left, 1)):
                with jax.named_scope("wait_l"):
                    wait(lbuf.at[par, h], l_recv.at[par, h])
                sbuf[par, slot, h] = _bf16(hold[h] + _f32(lbuf[par, h]))
                partial(slot, h, rbuf.at[i, slot, h], dev(nxt, chip, k), rs_recv.at[i]).start()

        @pl.when(last)
        def _():
            dst_stage = (CORES * i) // per_stage
            slot = lax.rem(CORES * i, per_stage) + k
            for r in range(ranks):
                mine = (dst_stage == p) & (r == t)

                @pl.when(mine)
                def _(r=r):
                    obuf[slot, c] = fbuf[par, r]

                @pl.when(jnp.logical_not(mine))
                def _(r=r):
                    remote(fbuf.at[par, r], obuf.at[slot, c], f_send.at[par, r], f_recv.at[slot, c],
                           {"pp": dst_stage, "tp": r}).start()
        at(8)

        @pl.when(idx + 1 == visits)
        def _():
            reduce_slab(idx + 1)
            forward(idx + 1)

        return carry

    lax.fori_loop(0, 2 * visits, visit, 0)

    with jax.named_scope("wait_out"):
        for j in range(per_stage):
            for q in range(chips):
                mine = at_end & (q == c) & (k == j % CORES)

                @pl.when(jnp.logical_not(mine))
                def _(j=j, q=q):
                    wait(obuf.at[j, q], f_recv.at[j, q])
            total = _f32(obuf[j, 0])
            for q in range(1, chips):
                total = total + _f32(obuf[j, q])
            out_ref[j] = _bf16(total)

    with jax.named_scope("wait_sends"):
        @pl.when(at_end)
        def _():
            for i in (visits - 2, visits - 1):
                f_wait(i)
        for par in range(2):
            wait(sbuf.at[par], rs_send.at[par])
            wait(ybuf.at[0, 0:3], ag_send.at[par])
        for v in range(2):
            for j in range(2):
                push_w(v, j).wait_send()

        @pl.when(jnp.logical_not(at_start))
        def _():
            x_load.wait()

        @pl.when(at_start)
        def _():
            wait(xs.at[0:visits], x_send.at[c])
            for chip in (far, right, left):
                wait(xs, x_send.at[chip])


def solution(mesh):
    stages, ranks = mesh.shape["pp"], mesh.shape["tp"]
    chips = ranks // CORES

    def per_device(x, gain, w_in, w_out):
        micro, tsh, width = x.shape
        passes, _, _, hid = w_in.shape
        tok = tsh * ranks
        visits = micro // CORES
        half = width // chips // 2
        per_stage = micro // stages
        dims = (stages, chips, visits, tok, width, hid)
        bf = jnp.bfloat16
        dma = pltpu.SemaphoreType.DMA
        any_space = pl.BlockSpec(memory_space=pl.ANY)
        vmem = pl.BlockSpec(memory_space=pltpu.VMEM)
        return pl.pallas_call(
            functools.partial(_kernel, dims),
            name="mlp_pipe",
            out_shape=jax.ShapeDtypeStruct((per_stage, tsh, width), bf),
            in_specs=[any_space, vmem, any_space, any_space],
            out_specs=vmem,
            scratch_shapes=[
                pltpu.VMEM((passes, CORES, width, hid), bf),
                pltpu.VMEM((passes, CORES, hid, width), bf),
                pltpu.VMEM((micro, tsh, width), bf),
                pltpu.VMEM((visits, ranks, tsh, width), bf),
                pltpu.VMEM((visits, chips, 2, tok, half), bf),
                pltpu.VMEM((visits, 3, 2, tok, half), bf),
                pltpu.VMEM((2, 2, tok, half), bf),
                pltpu.VMEM((2, tok, half), jnp.float32),
                pltpu.VMEM((tok, width), bf),
                pltpu.VMEM((CORES, tok, hid), bf),
                pltpu.VMEM((2, chips, 2, tok, half), bf),
                pltpu.VMEM((2, ranks, tsh, width), bf),
                pltpu.VMEM((per_stage, chips, tsh, width), bf),
                dma((passes, 2)), dma((passes, 2)), dma((passes, 2)),
                dma, dma((chips,)), dma((visits,)), pltpu.SemaphoreType.REGULAR,
                dma((2,)), dma((visits,)), dma((2, 2)), dma((2,)), dma((visits, 2)), dma((visits,)),
                dma((2, ranks)), dma((per_stage, chips)),
            ],
            compiler_params=pltpu.CompilerParams(collective_id=0, has_side_effects=True, vmem_limit_bytes=67043328),
        )(x, gain, w_in.reshape(passes, width, hid), w_out.reshape(passes, hid, width))

    return jax.shard_map(
        per_device,
        mesh=mesh,
        in_specs=(P("dp", "tp", None), P(None, "pp", None), P(None, "pp", None, "tp"), P(None, "pp", "tp", None)),
        out_specs=P(("dp", "pp"), "tp", None),
        check_vma=False,
    )
```

```python
import functools

import jax
import jax.numpy as jnp
from jax import lax
from jax.experimental import pallas as pl
from jax.experimental.pallas import tpu as pltpu
from jax.sharding import PartitionSpec as P

MESH = pl.DeviceIdType.MESH
NORM_EPS = 1e-5
CORES = 2
LOOKAHEAD = 2
REDUCE_AT = 4
LEAD_AT = 11
LEADS = 0
FORWARD_AT = 10
ADD_AT = 10
ADD_LEADS = 1
TILE = 256


def _f32(a):
    return a.astype(jnp.float32)


def _bf16(a):
    return a.astype(jnp.bfloat16)


def _kernel(dims, x_hbm, gain_ref, w1_hbm, w2_hbm, out_ref,
            w1, w2, xs, xbuf, ybuf, rbuf, stat, norm, lbuf, hold, hbuf, accb, abuf, sbuf, tbuf, obuf,
            wl_sem, wp_send, wp_recv, xl_sem, x_send, x_recv, ready,
            rs_send, rs_recv, l_recv, ag_send, ag_first, ag_near, ag_far, st_send, st_recv, o_send, o_recv):
    stages, chips, visits, tok, width, hid = dims
    ranks = chips * CORES
    slab = width // chips
    half = slab // 2
    tsh = tok // ranks
    per_stage = visits * CORES // stages
    p = lax.axis_index("pp")
    t = lax.axis_index("tp")
    c = t // CORES
    k = lax.rem(t, CORES)
    nxt = lax.rem(p + 1, stages)
    right, left = lax.rem(c + 1, chips), lax.rem(c + chips - 1, chips)
    far = lax.rem(c + 2, chips)
    at_start = p == 0
    at_end = p == stages - 1

    def dev(pp, chip, core):
        return {"pp": pp, "tp": chip * CORES + core}

    def remote(src, dst, ssem, rsem, where):
        return pltpu.make_async_remote_copy(src_ref=src, dst_ref=dst, send_sem=ssem, recv_sem=rsem,
                                            device_id=where, device_id_type=MESH)

    def wait(ref, sem):
        pltpu.make_async_copy(ref, ref, sem).wait()

    def load_w(v, j):
        src, dst = ((w1_hbm, w1), (w2_hbm, w2))[j]
        return pltpu.make_async_copy(src.at[v], dst.at[v, k], wl_sem.at[v, j])

    def push_w(v, j):
        src, dst = ((w1_hbm, w1), (w2_hbm, w2))[j]
        return remote(src.at[v], dst.at[v, k], wp_send.at[v, j], wp_recv.at[v, j], dev(p, c, 1 - k))

    x_load = pltpu.make_async_copy(x_hbm, xs, xl_sem)
    x_load.start()
    for v in range(2):
        for j in range(2):
            load_w(v, j).start()

    bar = pltpu.get_barrier_semaphore()
    for r in range(ranks):
        @pl.when(r != t)
        def _(r=r):
            pl.semaphore_signal(bar, inc=1, device_id={"pp": p, "tp": r}, device_id_type=MESH)

    @pl.when(jnp.logical_not(at_end))
    def _():
        for q in range(chips):
            pl.semaphore_signal(bar, inc=1, device_id=dev(nxt, q, k), device_id_type=MESH)
    pl.semaphore_wait(bar, jnp.where(at_start, ranks - 1, ranks - 1 + chips))

    @pl.when(jnp.logical_not(at_start))
    def _():
        for q in range(chips):
            pl.semaphore_signal(ready, inc=1, device_id=dev(p - 1, q, k), device_id_type=MESH)

    def x_copy(i, core, chip):
        return remote(xs.at[CORES * i + core], xbuf.at[i, t], x_send.at[chip], x_recv.at[i], dev(p, chip, core))

    def x_share(i):
        xbuf[i, t] = xs[CORES * i + k]
        for core in range(CORES):
            for chip in (far, right, left):
                x_copy(i, core, chip).start()

    @pl.when(at_start)
    def _():
        x_load.wait()
        for i in range(visits):
            x_copy(i, 1 - k, c).start()
        for i in range(LOOKAHEAD):
            x_share(i)

    for v in range(2):
        for j in range(2):
            push_w(v, j).start()

    def share(i, par, owner, h, chip, sem):
        return remote(ybuf.at[i, owner, h], ybuf.at[i, owner, h], ag_send.at[par], sem, dev(p, chip, k))

    def reduce_slab(idx):
        i = lax.rem(idx, visits)
        par = lax.rem(idx, 2)

        @pl.when(idx >= jnp.where(at_start, visits + 2, 2))
        def _():
            wait(ybuf.at[i, 0:3], ag_send.at[par])
            wait(stat.at[i, 0:3], st_send.at[par])

        with jax.named_scope("wait_rs"):
            wait(rbuf.at[i], rs_recv.at[i])
        own = [_bf16(_f32(rbuf[i, 0, h]) + _f32(rbuf[i, 1, h]) + _f32(rbuf[i, 2, h])) for h in range(2)]
        for h in range(2):
            ybuf[i, c, h] = own[h]
        own = [_f32(a) for a in own]
        mean = sum(jnp.sum(a, axis=-1, keepdims=True) for a in own) * (1.0 / slab)
        dev2 = sum(jnp.sum((a - mean) * (a - mean), axis=-1, keepdims=True) for a in own)
        lane = lax.broadcasted_iota(jnp.int32, (8, 128), 1)
        for j, col in enumerate((mean, dev2)):
            tile = jnp.zeros((8, 128), jnp.float32)
            for a in range(tok // 8):
                tile = jnp.where(lane == a, col[8 * a:8 * a + 8, :], tile)
            stat[i, c, j] = tile
        for chip in (far, right, left):
            remote(stat.at[i, c], stat.at[i, c], st_send.at[par], st_recv.at[i], dev(p, chip, k)).start()
        share(i, par, c, 0, right, ag_first.at[i, 0]).start()
        share(i, par, c, 1, left, ag_first.at[i, 1]).start()
        share(i, par, c, 1, right, ag_near.at[i]).start()
        share(i, par, c, 0, left, ag_near.at[i]).start()

    def forward(idx):
        i = lax.rem(idx, visits)
        par = lax.rem(idx, 2)
        with jax.named_scope("wait_fwd"):
            wait(ybuf.at[i, left, 0], ag_first.at[i, 0])
            share(i, par, left, 0, right, ag_far.at[i]).start()
            wait(ybuf.at[i, right, 1], ag_first.at[i, 1])
            share(i, par, right, 1, left, ag_far.at[i]).start()

    @pl.when(jnp.logical_not(at_start))
    def _():
        reduce_slab(0)
        forward(0)

    def add_relayed(idx):
        i = lax.rem(idx, visits)
        par = lax.rem(idx, 2)
        dst = jnp.where(at_end & (idx >= visits), CORES * i // per_stage, nxt)
        for slot, chip, h in ((1, right, 0), (2, left, 1)):
            got = lax.rem(idx, 3)
            with jax.named_scope("wait_l"):
                wait(lbuf.at[got, h], l_recv.at[got, h])
            sbuf[par, slot, h] = _bf16(hold[par, h] + _f32(lbuf[got, h]))
            remote(sbuf.at[par, slot, h], rbuf.at[i, slot, h], rs_send.at[par], rs_recv.at[i], dev(dst, chip, k)).start()

    def visit(kind, idx, carry):
        v = 0 if kind == "first" else idx // visits
        i = lax.rem(idx, visits)
        dst = jnp.where(at_end & (v == 1), CORES * i // per_stage, nxt)
        par = lax.rem(idx, 2)

        def at(place):
            if place == ADD_AT and place < 10:
                @pl.when(i > ADD_LEADS)
                def _():
                    add_relayed(idx - 1)
            if kind == "first":
                return
            ahead = (idx + 1 < 2 * visits) & (idx + 1 != visits)
            if place == REDUCE_AT:
                @pl.when(ahead & (i >= LEADS))
                def _():
                    reduce_slab(idx + 1)
            if place == LEAD_AT:
                @pl.when(ahead & (i < LEADS))
                def _():
                    reduce_slab(idx + 1)
            if place == FORWARD_AT:
                @pl.when(ahead & (i >= LEADS))
                def _():
                    forward(idx + 1)

        if kind == "first":
            @pl.when(i + LOOKAHEAD < visits)
            def _():
                x_share(i + LOOKAHEAD)
            with jax.named_scope("wait_x"):
                wait(xbuf.at[i, 0:ranks - 1], x_recv.at[i])
            for q in range(chips):
                for h in range(2):
                    lo = q * slab + h * half
                    ybuf[i, q, h] = _bf16(_f32(xbuf[i, :, :, lo:lo + half]).reshape(tok, half))

        at(1)

        def keep(mean, scale):
            norm[0] = jnp.broadcast_to(mean, (tok, 128))
            norm[1] = jnp.broadcast_to(scale, (tok, 128))

        if kind == "first":
            pieces = [(q, h) for q in range(chips) for h in range(2)]
            mean = sum(jnp.sum(_f32(ybuf[i, q, h]), axis=-1, keepdims=True) for q, h in pieces) * (1.0 / width)
            var = jnp.zeros_like(mean)
            for q, h in pieces:
                a = _f32(ybuf[i, q, h]) - mean
                var = var + jnp.sum(a * a, axis=-1, keepdims=True)
            keep(mean, lax.rsqrt(var * (1.0 / width) + NORM_EPS))

        else:
            with jax.named_scope("wait_st"):
                wait(stat.at[i, 0:3], st_recv.at[i])
            means = [stat[i, q, 0] for q in range(chips)]
            mean = sum(means) * (1.0 / chips)
            dev2 = sum(stat[i, q, 1] + slab * (means[q] - mean) * (means[q] - mean) for q in range(chips))
            scale = lax.rsqrt(dev2 * (1.0 / width) + NORM_EPS)
            for a in range(tok // 8):
                rows = slice(8 * a, 8 * a + 8)
                norm[0, rows] = jnp.broadcast_to(mean[:, a:a + 1], (8, 128))
                norm[1, rows] = jnp.broadcast_to(scale[:, a:a + 1], (8, 128))

        def wait_weights(j):
            @pl.when(i == 0)
            def _():
                load_w(v, j).wait()
                push_w(v, j).wait_recv()

        with jax.named_scope("wait_w1"):
            wait_weights(0)
        at(2)
        tile = TILE
        for n_done, chip in enumerate((c, right, left, far)):
            if n_done in (1, 3) and kind != "first":
                with jax.named_scope("wait_ag"):
                    wait(ybuf.at[i, 0], (None, ag_near, None, ag_far)[n_done].at[i])
            for m in range(slab // 128):
                cols = slice(m * 128, (m + 1) * 128)
                gain = gain_ref[v, :, pl.ds(pl.multiple_of(chip * slab + m * 128, 128), 128)]
                h, lo = m * 128 // half, m * 128 % half
                hbuf[:, cols] = _bf16((_f32(ybuf[i, chip, h, :, lo:lo + 128]) - norm[0]) * norm[1] * _f32(gain))
            for s in range(CORES):
                for col in range(0, hid, 2 * tile):
                    rows = pl.ds(pl.multiple_of(chip * slab, slab), slab)
                    cols = slice(col, col + 2 * tile)
                    part = jnp.dot(hbuf[...], w1[v, s, rows, cols], preferred_element_type=jnp.float32)
                    if n_done:
                        part = part + accb[s, :, cols]
                    if n_done < 3:
                        accb[s, :, cols] = part
                    else:
                        abuf[s, :, cols] = _bf16(jax.nn.gelu(part))
            if n_done < 3:
                at(3 + n_done)
        at(6)
        with jax.named_scope("wait_w2"):
            wait_weights(1)

        @pl.when(idx == 0)
        def _():
            @pl.when(jnp.logical_not(at_end))
            def _():
                pl.semaphore_wait(ready, chips)

        @pl.when(idx >= 2)
        def _():
            wait(sbuf.at[par], rs_send.at[par])

        def partial(slot, h, dst, where, sem):
            return remote(sbuf.at[par, slot, h], dst, rs_send.at[par], sem, where)

        def slab_done(n, q, prod):
            prod = prod[:, :half], prod[:, half:]
            if n == 0:
                got = lax.rem(idx, 3)
                for h, chip in ((0, right), (1, left)):
                    sbuf[par, 0, h] = _bf16(prod[h])
                    partial(0, h, lbuf.at[got, h], dev(p, chip, k), l_recv.at[got, h]).start()
            elif n == 3:
                for h in range(2):
                    sbuf[par, 3, h] = _bf16(prod[h] + _f32(ybuf[i, c, h]))


                @pl.when(dst != p)
                def _():
                    remote(sbuf.at[par, 3], rbuf.at[i, 0], rs_send.at[par], rs_recv.at[i], dev(dst, c, k)).start()

                @pl.when(dst == p)
                def _():
                    rbuf[i, 0] = sbuf[par, 3]
            else:
                h = 2 - n
                sbuf[par, n, h] = _bf16(prod[h])
                hold[par, 1 - h] = prod[1 - h]
                partial(n, h, rbuf.at[i, n, h], dev(dst, q, k), rs_recv.at[i]).start()

        order = (far, right, left, c)
        for n, q in enumerate(order):
            cols = pl.ds(pl.multiple_of(q * slab, slab), slab)
            prod = jnp.zeros((tok, slab), jnp.float32)
            for s in range(CORES):
                prod = prod + _f32(_bf16(jnp.dot(abuf[s], w2[v, s, :, cols], preferred_element_type=jnp.float32)))
            slab_done(n, q, prod)
            if n < 3:
                at(7 + n)
        at(10)
        @pl.when((i < ADD_LEADS) | (i == visits - 1) | (ADD_AT > 9))
        def _():
            add_relayed(idx)
        at(11)
        if kind == "mid":
            @pl.when((i < LEADS) & (idx + 1 < 2 * visits) & (idx + 1 != visits))
            def _():
                forward(idx + 1)

        @pl.when(idx + 1 == visits)
        def _():
            reduce_slab(idx + 1)
            forward(idx + 1)

        return carry

    mid_from = jnp.where(at_start, visits, 0)
    lax.fori_loop(0, mid_from, functools.partial(visit, "first"), 0)
    lax.fori_loop(mid_from, 2 * visits, functools.partial(visit, "mid"), 0)

    per_core = per_stage // CORES
    with jax.named_scope("wait_out"):
        for n in range(per_core):
            i = per_core * p + n
            j = CORES * n + k

            @pl.when(at_end)
            def _(i=i):
                wait(rbuf.at[i, 0:2], rs_recv.at[i])

            @pl.when(jnp.logical_not(at_end))
            def _(i=i):
                wait(rbuf.at[i], rs_recv.at[i])
            for h in range(2):
                total = _bf16(_f32(rbuf[i, 0, h]) + _f32(rbuf[i, 1, h]) + _f32(rbuf[i, 2, h]))
                tbuf[n, :, :, h * half:(h + 1) * half] = _bf16(_f32(total).reshape(ranks, tsh, half))
            for r in range(ranks):
                @pl.when(r == t)
                def _(r=r, n=n, j=j):
                    obuf[j, c] = tbuf[n, r]

                @pl.when(r != t)
                def _(r=r, n=n, j=j):
                    remote(tbuf.at[n, r], obuf.at[j, c], o_send.at[n], o_recv.at[j], {"pp": p, "tp": r}).start()
    with jax.named_scope("wait_out2"):
        for j in range(per_stage):
            @pl.when(j % CORES == k)
            def _(j=j):
                wait(obuf.at[j, 0:chips - 1], o_recv.at[j])

            @pl.when(j % CORES != k)
            def _(j=j):
                wait(obuf.at[j], o_recv.at[j])
            for q in range(chips):
                out_ref[j, :, q * slab:(q + 1) * slab] = obuf[j, q]

    with jax.named_scope("wait_sends"):
        for n in range(per_core):
            wait(tbuf.at[n, 0:ranks - 1], o_send.at[n])
        for par in range(2):
            @pl.when(at_end)
            def _(par=par):
                wait(sbuf.at[par, 0:3], rs_send.at[par])

            @pl.when(jnp.logical_not(at_end))
            def _(par=par):
                wait(sbuf.at[par], rs_send.at[par])
            wait(ybuf.at[0, 0:3], ag_send.at[par])
            wait(stat.at[0, 0:3], st_send.at[par])
        for v in range(2):
            for j in range(2):
                push_w(v, j).wait_send()

        @pl.when(jnp.logical_not(at_start))
        def _():
            x_load.wait()

        @pl.when(at_start)
        def _():
            wait(xs.at[0:visits], x_send.at[c])
            for chip in (far, right, left):
                wait(xs, x_send.at[chip])


def solution(mesh):
    stages, ranks = mesh.shape["pp"], mesh.shape["tp"]
    chips = ranks // CORES

    def per_device(x, gain, w_in, w_out):
        micro, tsh, width = x.shape
        passes, _, _, hid = w_in.shape
        tok = tsh * ranks
        visits = micro // CORES
        half = width // chips // 2
        per_stage = micro // stages
        dims = (stages, chips, visits, tok, width, hid)
        bf = jnp.bfloat16
        dma = pltpu.SemaphoreType.DMA
        any_space = pl.BlockSpec(memory_space=pl.ANY)
        vmem = pl.BlockSpec(memory_space=pltpu.VMEM)
        return pl.pallas_call(
            functools.partial(_kernel, dims),
            name="mlp_pipe",
            out_shape=jax.ShapeDtypeStruct((per_stage, tsh, width), bf),
            in_specs=[any_space, vmem, any_space, any_space],
            out_specs=vmem,
            scratch_shapes=[
                pltpu.VMEM((passes, CORES, width, hid), bf),
                pltpu.VMEM((passes, CORES, hid, width), bf),
                pltpu.VMEM((micro, tsh, width), bf),
                pltpu.VMEM((visits, ranks, tsh, width), bf),
                pltpu.VMEM((visits, chips, 2, tok, half), bf),
                pltpu.VMEM((visits, 3, 2, tok, half), bf),
                pltpu.VMEM((visits, chips, 2, 8, 128), jnp.float32),
                pltpu.VMEM((2, tok, 128), jnp.float32),
                pltpu.VMEM((3, 2, tok, half), bf),
                pltpu.VMEM((2, 2, tok, half), jnp.float32),
                pltpu.VMEM((tok, 2 * half), bf),
                pltpu.VMEM((CORES, tok, hid), jnp.float32),
                pltpu.VMEM((CORES, tok, hid), bf),
                pltpu.VMEM((2, chips, 2, tok, half), bf),
                pltpu.VMEM((per_stage // CORES, ranks, tsh, 2 * half), bf),
                pltpu.VMEM((per_stage, chips, tsh, 2 * half), bf),
                dma((passes, 2)), dma((passes, 2)), dma((passes, 2)),
                dma, dma((chips,)), dma((visits,)), pltpu.SemaphoreType.REGULAR,
                dma((2,)), dma((visits,)), dma((3, 2)), dma((2,)), dma((visits, 2)), dma((visits,)), dma((visits,)), dma((2,)), dma((visits,)),
                dma((per_stage // CORES,)), dma((per_stage,)),
            ],
            compiler_params=pltpu.CompilerParams(collective_id=0, has_side_effects=True, vmem_limit_bytes=67043328),
        )(x, gain, w_in.reshape(passes, width, hid), w_out.reshape(passes, hid, width))

    return jax.shard_map(
        per_device,
        mesh=mesh,
        in_specs=(P("dp", "tp", None), P(None, "pp", None), P(None, "pp", None, "tp"), P(None, "pp", "tp", None)),
        out_specs=P(("dp", "pp"), "tp", None),
        check_vma=False,
    )
```

```python
import functools

import jax
import jax.numpy as jnp
from jax import lax
from jax.experimental import pallas as pl
from jax.experimental.pallas import tpu as pltpu
from jax.sharding import PartitionSpec as P

MESH = pl.DeviceIdType.MESH
NORM_EPS = 1e-5
CORES = 2
LOOKAHEAD = 2
REDUCE_AT = 4
LEAD_AT = 11
LEADS = 0
FORWARD_AT = 10
FLAGS = {}
ADD_AT = 10
ADD_LEADS = 1
TILE = 256


def _f32(a):
    return a.astype(jnp.float32)


def _bf16(a):
    return a.astype(jnp.bfloat16)


def _kernel(dims, x_hbm, gain_ref, w1_hbm, w2_hbm, out_ref,
            w1, w2, xs, xbuf, ybuf, rbuf, stat, norm, lbuf, hold, hbuf, accb, hx, qbuf, qrecv, abuf, sbuf, tbuf, obuf,
            wl_sem, wp_send, wp_recv, xl_sem, x_send, x_recv, ready,
            rs_send, rs_recv, l_recv, ag_send, ag_first, ag_near, ag_far, st_send, st_recv, o_send, o_recv, h_send, h_recv, q_send, q_recv):
    stages, chips, visits, tok, width, hid = dims
    ranks = chips * CORES
    slab = width // chips
    half = slab // 2
    tsh = tok // ranks
    per_stage = visits * CORES // stages
    p = lax.axis_index("pp")
    t = lax.axis_index("tp")
    c = t // CORES
    k = lax.rem(t, CORES)
    nxt = lax.rem(p + 1, stages)
    right, left = lax.rem(c + 1, chips), lax.rem(c + chips - 1, chips)
    far = lax.rem(c + 2, chips)
    at_start = p == 0
    at_end = p == stages - 1

    def dev(pp, chip, core):
        return {"pp": pp, "tp": chip * CORES + core}

    def remote(src, dst, ssem, rsem, where):
        return pltpu.make_async_remote_copy(src_ref=src, dst_ref=dst, send_sem=ssem, recv_sem=rsem,
                                            device_id=where, device_id_type=MESH)

    def wait(ref, sem):
        pltpu.make_async_copy(ref, ref, sem).wait()

    def load_w(v, j):
        src, dst = ((w1_hbm, w1), (w2_hbm, w2))[j]
        return pltpu.make_async_copy(src.at[v], dst.at[v, k], wl_sem.at[v, j])

    def push_w(v, j):
        src, dst = ((w1_hbm, w1), (w2_hbm, w2))[j]
        return remote(src.at[v], dst.at[v, k], wp_send.at[v, j], wp_recv.at[v, j], dev(p, c, 1 - k))

    def push_piece(i):
        for j, (src, dst) in enumerate(((w1_hbm, w1), (w2_hbm, w2))):
            size = src.shape[1] // visits
            rows = pl.ds(pl.multiple_of(i * size, size), size)
            remote(src.at[1, rows], dst.at[1, k, rows], wp_send.at[1, j], wp_recv.at[1, j], dev(p, c, 1 - k)).start()

    x_load = pltpu.make_async_copy(x_hbm, xs, xl_sem)
    x_load.start()
    for v in range(2):
        for j in range(2):
            load_w(v, j).start()

    bar = pltpu.get_barrier_semaphore()
    for r in range(ranks):
        @pl.when(r != t)
        def _(r=r):
            pl.semaphore_signal(bar, inc=1, device_id={"pp": p, "tp": r}, device_id_type=MESH)

    @pl.when(jnp.logical_not(at_end))
    def _():
        for q in range(chips):
            pl.semaphore_signal(bar, inc=1, device_id=dev(nxt, q, k), device_id_type=MESH)
    pl.semaphore_wait(bar, jnp.where(at_start, ranks - 1, ranks - 1 + chips))

    @pl.when(jnp.logical_not(at_start))
    def _():
        for q in range(chips):
            pl.semaphore_signal(ready, inc=1, device_id=dev(p - 1, q, k), device_id_type=MESH)

    def x_copy(i, core, chip):
        return remote(xs.at[CORES * i + core], xbuf.at[i, t], x_send.at[chip], x_recv.at[i], dev(p, chip, core))

    def x_share(i):
        xbuf[i, t] = xs[CORES * i + k]
        for core in range(CORES):
            for chip in (far, right, left):
                x_copy(i, core, chip).start()

    @pl.when(at_start)
    def _():
        x_load.wait()
        for i in range(visits):
            x_copy(i, 1 - k, c).start()
        for i in range(LOOKAHEAD):
            x_share(i)

    @pl.when(jnp.logical_not(at_start))
    def _():
        for v in range(2):
            for j in range(2):
                push_w(v, j).start()

    def share(i, par, owner, h, chip, sem):
        return remote(ybuf.at[i, owner, h], ybuf.at[i, owner, h], ag_send.at[par], sem, dev(p, chip, k))

    def reduce_slab(idx):
        i = lax.rem(idx, visits)
        par = lax.rem(idx, 2)

        @pl.when(idx >= jnp.where(at_start, visits + 2, 2))
        def _():
            wait(ybuf.at[i, 0:3], ag_send.at[par])
            wait(stat.at[i, 0:3], st_send.at[par])

        with jax.named_scope("wait_rs"):
            wait(rbuf.at[i], rs_recv.at[i])
        own = [_bf16(_f32(rbuf[i, 0, h]) + _f32(rbuf[i, 1, h]) + _f32(rbuf[i, 2, h])) for h in range(2)]
        for h in range(2):
            ybuf[i, c, h] = own[h]
        own = [_f32(a) for a in own]
        mean = sum(jnp.sum(a, axis=-1, keepdims=True) for a in own) * (1.0 / slab)
        dev2 = sum(jnp.sum((a - mean) * (a - mean), axis=-1, keepdims=True) for a in own)
        lane = lax.broadcasted_iota(jnp.int32, (8, 128), 1)
        for j, col in enumerate((mean, dev2)):
            tile = jnp.zeros((8, 128), jnp.float32)
            for a in range(tok // 8):
                tile = jnp.where(lane == a, col[8 * a:8 * a + 8, :], tile)
            stat[i, c, j] = tile
        for chip in (far, right, left):
            remote(stat.at[i, c], stat.at[i, c], st_send.at[par], st_recv.at[i], dev(p, chip, k)).start()
        share(i, par, c, 0, right, ag_first.at[i, 0]).start()
        share(i, par, c, 1, left, ag_first.at[i, 1]).start()
        share(i, par, c, 1, right, ag_near.at[i]).start()
        share(i, par, c, 0, left, ag_near.at[i]).start()

    def forward(idx):
        i = lax.rem(idx, visits)
        par = lax.rem(idx, 2)
        with jax.named_scope("wait_fwd"):
            wait(ybuf.at[i, left, 0], ag_first.at[i, 0])
            share(i, par, left, 0, right, ag_far.at[i]).start()
            wait(ybuf.at[i, right, 1], ag_first.at[i, 1])
            share(i, par, right, 1, left, ag_far.at[i]).start()

    @pl.when(jnp.logical_not(at_start))
    def _():
        reduce_slab(0)
        forward(0)

    def add_relayed(idx):
        i = lax.rem(idx, visits)
        par = lax.rem(idx, 2)
        dst = jnp.where(at_end & (idx >= visits), CORES * i // per_stage, nxt)
        for slot, chip, h in ((1, right, 0), (2, left, 1)):
            got = lax.rem(idx, 3)
            with jax.named_scope("wait_l"):
                wait(lbuf.at[got, h], l_recv.at[got, h])
            sbuf[par, slot, h] = _bf16(hold[par, h] + _f32(lbuf[got, h]))
            remote(sbuf.at[par, slot, h], rbuf.at[i, slot, h], rs_send.at[par], rs_recv.at[i], dev(dst, chip, k)).start()

    def visit(kind, idx, carry):
        v = 0 if kind == "first" else idx // visits
        i = lax.rem(idx, visits)
        dst = jnp.where(at_end & (v == 1), CORES * i // per_stage, nxt)
        par = lax.rem(idx, 2)

        def at(place):
            if place == ADD_AT and place < 10:
                @pl.when(i > ADD_LEADS)
                def _():
                    add_relayed(idx - 1)
            if kind == "first":
                return
            ahead = (idx + 1 < 2 * visits) & (idx + 1 != visits)
            if place == REDUCE_AT:
                @pl.when(ahead & (i >= LEADS))
                def _():
                    reduce_slab(idx + 1)
            if place == LEAD_AT:
                @pl.when(ahead & (i < LEADS))
                def _():
                    reduce_slab(idx + 1)
            if place == FORWARD_AT:
                @pl.when(ahead & (i >= LEADS))
                def _():
                    forward(idx + 1)

        if kind == "first":
            @pl.when(i + LOOKAHEAD < visits)
            def _():
                x_share(i + LOOKAHEAD)
            with jax.named_scope("wait_x"):
                wait(xbuf.at[i, 0:ranks - 1], x_recv.at[i])
            for q in range(chips):
                for h in range(2):
                    lo = q * slab + h * half
                    ybuf[i, q, h] = _bf16(_f32(xbuf[i, :, :, lo:lo + half]).reshape(tok, half))

        at(1)

        def keep(mean, scale):
            norm[0] = jnp.broadcast_to(mean, (tok, 128))
            norm[1] = jnp.broadcast_to(scale, (tok, 128))

        if kind == "first":
            pieces = [(q, h) for q in range(chips) for h in range(2)]
            mean = sum(jnp.sum(_f32(ybuf[i, q, h]), axis=-1, keepdims=True) for q, h in pieces) * (1.0 / width)
            var = jnp.zeros_like(mean)
            for q, h in pieces:
                a = _f32(ybuf[i, q, h]) - mean
                var = var + jnp.sum(a * a, axis=-1, keepdims=True)
            keep(mean, lax.rsqrt(var * (1.0 / width) + NORM_EPS))

        else:
            with jax.named_scope("wait_st"):
                wait(stat.at[i, 0:3], st_recv.at[i])
            means = [stat[i, q, 0] for q in range(chips)]
            mean = sum(means) * (1.0 / chips)
            dev2 = sum(stat[i, q, 1] + slab * (means[q] - mean) * (means[q] - mean) for q in range(chips))
            scale = lax.rsqrt(dev2 * (1.0 / width) + NORM_EPS)
            for a in range(tok // 8):
                rows = slice(8 * a, 8 * a + 8)
                norm[0, rows] = jnp.broadcast_to(mean[:, a:a + 1], (8, 128))
                norm[1, rows] = jnp.broadcast_to(scale[:, a:a + 1], (8, 128))

        def wait_weights(j):
            @pl.when(i == 0)
            def _():
                load_w(v, j).wait()
                if kind != "first":
                    push_w(v, j).wait_recv()

        with jax.named_scope("wait_w1"):
            wait_weights(0)
        at(2)
        tile = TILE
        if kind == "first":
            @pl.when(i > 0)
            def _():
                wait(hx.at[0], h_send)
            for q in range(chips):
                for m in range(slab // 128):
                    cols = slice(q * slab + m * 128, q * slab + (m + 1) * 128)
                    h, lo = m * 128 // half, m * 128 % half
                    hx[k, :, cols] = _bf16((_f32(ybuf[i, q, h, :, lo:lo + 128]) - norm[0]) * norm[1] * _f32(gain_ref[v, :, cols]))
            remote(hx.at[k], hx.at[k], h_send, h_recv, dev(p, c, 1 - k)).start()

            @pl.when(i > 0)
            def _():
                add_relayed(idx - 1)
            with jax.named_scope("wait_h"):
                wait(hx.at[0], h_recv)
            for col in range(0, hid, 2 * tile):
                cols = slice(col, col + 2 * tile)
                part = jnp.dot(hx[...].reshape(CORES * tok, width), w1[v, k, :, cols], preferred_element_type=jnp.float32)
                abuf[:, :, cols] = _bf16(jax.nn.gelu(part)).reshape(CORES, tok, 2 * tile)
        for n_done, chip in enumerate((c, right, left, far) if kind != "first" else ()):
            if n_done in (1, 3):
                with jax.named_scope("wait_ag"):
                    wait(ybuf.at[i, 0], (None, ag_near, None, ag_far)[n_done].at[i])
            for m in range(slab // 128):
                cols = slice(m * 128, (m + 1) * 128)
                gain = gain_ref[v, :, pl.ds(pl.multiple_of(chip * slab + m * 128, 128), 128)]
                h, lo = m * 128 // half, m * 128 % half
                hbuf[:, cols] = _bf16((_f32(ybuf[i, chip, h, :, lo:lo + 128]) - norm[0]) * norm[1] * _f32(gain))
            for s in range(CORES):
                for col in range(0, hid, 2 * tile):
                    rows = pl.ds(pl.multiple_of(chip * slab, slab), slab)
                    cols = slice(col, col + 2 * tile)
                    part = jnp.dot(hbuf[...], w1[v, s, rows, cols], preferred_element_type=jnp.float32)
                    if n_done:
                        part = part + accb[s, :, cols]
                    if n_done < 3:
                        accb[s, :, cols] = part
                    else:
                        abuf[s, :, cols] = _bf16(jax.nn.gelu(part))
            if n_done < 3:
                at(3 + n_done)
        at(6)
        with jax.named_scope("wait_w2"):
            wait_weights(1)

        @pl.when(idx == 0)
        def _():
            @pl.when(jnp.logical_not(at_end))
            def _():
                pl.semaphore_wait(ready, chips)

        @pl.when(idx >= 2)
        def _():
            wait(sbuf.at[par], rs_send.at[par])

        def partial(slot, h, dst, where, sem):
            return remote(sbuf.at[par, slot, h], dst, rs_send.at[par], sem, where)

        def slab_done(n, q, prod):
            prod = prod[:, :half], prod[:, half:]
            if n == 0:
                got = lax.rem(idx, 3)
                for h, chip in ((0, right), (1, left)):
                    sbuf[par, 0, h] = _bf16(prod[h])
                    partial(0, h, lbuf.at[got, h], dev(p, chip, k), l_recv.at[got, h]).start()
            elif n == 3:
                for h in range(2):
                    sbuf[par, 3, h] = _bf16(prod[h] + _f32(ybuf[i, c, h]))


                @pl.when(dst != p)
                def _():
                    remote(sbuf.at[par, 3], rbuf.at[i, 0], rs_send.at[par], rs_recv.at[i], dev(dst, c, k)).start()

                @pl.when(dst == p)
                def _():
                    rbuf[i, 0] = sbuf[par, 3]
            else:
                h = 2 - n
                sbuf[par, n, h] = _bf16(prod[h])
                hold[par, 1 - h] = prod[1 - h]
                partial(n, h, rbuf.at[i, n, h], dev(dst, q, k), rs_recv.at[i]).start()

        order = (far, right, left, c)
        if kind == "first":
            @pl.when(i > 0)
            def _():
                wait(qrecv, q_send)
            for n, q in enumerate(order):
                cols = pl.ds(pl.multiple_of(q * slab, slab), slab)
                prod = jnp.dot(abuf[...].reshape(CORES * tok, hid), w2[v, k, :, cols], preferred_element_type=jnp.float32)
                qbuf[n] = _bf16(prod).reshape(CORES, tok, slab)
                remote(qbuf.at[n, 1 - k], qrecv.at[n], q_send, q_recv.at[n], dev(p, c, 1 - k)).start()
            for n, q in enumerate(order):
                with jax.named_scope("wait_q"):
                    wait(qrecv.at[n], q_recv.at[n])
                slab_done(n, q, _f32(qbuf[n, k]) + _f32(qrecv[n]))
            push_piece(i)
        for n, q in enumerate(order if kind != "first" else ()):
            cols = pl.ds(pl.multiple_of(q * slab, slab), slab)
            prod = jnp.zeros((tok, slab), jnp.float32)
            for s in range(CORES):
                prod = prod + _f32(_bf16(jnp.dot(abuf[s], w2[v, s, :, cols], preferred_element_type=jnp.float32)))
            slab_done(n, q, prod)
            if n < 3:
                at(7 + n)
        at(10)
        @pl.when((i == visits - 1) if kind == "first" else (i < ADD_LEADS) | (i == visits - 1) | (ADD_AT > 9))
        def _():
            add_relayed(idx)
        at(11)
        if kind == "mid":
            @pl.when((i < LEADS) & (idx + 1 < 2 * visits) & (idx + 1 != visits))
            def _():
                forward(idx + 1)

        @pl.when(idx + 1 == visits)
        def _():
            reduce_slab(idx + 1)
            forward(idx + 1)

        return carry

    mid_from = jnp.where(at_start, visits, 0)
    lax.fori_loop(0, mid_from, functools.partial(visit, "first"), 0)
    lax.fori_loop(mid_from, 2 * visits, functools.partial(visit, "mid"), 0)

    per_core = per_stage // CORES
    with jax.named_scope("wait_out"):
        for n in range(per_core):
            i = per_core * p + n
            j = CORES * n + k

            @pl.when(at_end)
            def _(i=i):
                wait(rbuf.at[i, 0:2], rs_recv.at[i])

            @pl.when(jnp.logical_not(at_end))
            def _(i=i):
                wait(rbuf.at[i], rs_recv.at[i])
            for h in range(2):
                total = _bf16(_f32(rbuf[i, 0, h]) + _f32(rbuf[i, 1, h]) + _f32(rbuf[i, 2, h]))
                tbuf[n, :, :, h * half:(h + 1) * half] = _bf16(_f32(total).reshape(ranks, tsh, half))
            for r in range(ranks):
                @pl.when(r == t)
                def _(r=r, n=n, j=j):
                    obuf[j, c] = tbuf[n, r]

                @pl.when(r != t)
                def _(r=r, n=n, j=j):
                    remote(tbuf.at[n, r], obuf.at[j, c], o_send.at[n], o_recv.at[j], {"pp": p, "tp": r}).start()
    with jax.named_scope("wait_out2"):
        for j in range(per_stage):
            @pl.when(j % CORES == k)
            def _(j=j):
                wait(obuf.at[j, 0:chips - 1], o_recv.at[j])

            @pl.when(j % CORES != k)
            def _(j=j):
                wait(obuf.at[j], o_recv.at[j])
            for q in range(chips):
                out_ref[j, :, q * slab:(q + 1) * slab] = obuf[j, q]

    with jax.named_scope("wait_sends"):
        @pl.when(at_start)
        def _():
            wait(hx.at[0], h_send)
            wait(qrecv, q_send)
        for n in range(per_core):
            wait(tbuf.at[n, 0:ranks - 1], o_send.at[n])
        for par in range(2):
            @pl.when(at_end)
            def _(par=par):
                wait(sbuf.at[par, 0:3], rs_send.at[par])

            @pl.when(jnp.logical_not(at_end))
            def _(par=par):
                wait(sbuf.at[par], rs_send.at[par])
            wait(ybuf.at[0, 0:3], ag_send.at[par])
            wait(stat.at[0, 0:3], st_send.at[par])
        for v in range(2):
            @pl.when((v == 1) | jnp.logical_not(at_start))
            def _(v=v):
                for j in range(2):
                    push_w(v, j).wait_send()

        @pl.when(jnp.logical_not(at_start))
        def _():
            x_load.wait()

        @pl.when(at_start)
        def _():
            wait(xs.at[0:visits], x_send.at[c])
            for chip in (far, right, left):
                wait(xs, x_send.at[chip])


def solution(mesh):
    stages, ranks = mesh.shape["pp"], mesh.shape["tp"]
    chips = ranks // CORES

    def per_device(x, gain, w_in, w_out):
        micro, tsh, width = x.shape
        passes, _, _, hid = w_in.shape
        tok = tsh * ranks
        visits = micro // CORES
        half = width // chips // 2
        per_stage = micro // stages
        dims = (stages, chips, visits, tok, width, hid)
        bf = jnp.bfloat16
        dma = pltpu.SemaphoreType.DMA
        any_space = pl.BlockSpec(memory_space=pl.ANY)
        vmem = pl.BlockSpec(memory_space=pltpu.VMEM)
        return pl.pallas_call(
            functools.partial(_kernel, dims),
            name="mlp_pipe",
            out_shape=jax.ShapeDtypeStruct((per_stage, tsh, width), bf),
            in_specs=[any_space, vmem, any_space, any_space],
            out_specs=vmem,
            scratch_shapes=[
                pltpu.VMEM((passes, CORES, width, hid), bf),
                pltpu.VMEM((passes, CORES, hid, width), bf),
                pltpu.VMEM((micro, tsh, width), bf),
                pltpu.VMEM((visits, ranks, tsh, width), bf),
                pltpu.VMEM((visits, chips, 2, tok, half), bf),
                pltpu.VMEM((visits, 3, 2, tok, half), bf),
                pltpu.VMEM((visits, chips, 2, 8, 128), jnp.float32),
                pltpu.VMEM((2, tok, 128), jnp.float32),
                pltpu.VMEM((3, 2, tok, half), bf),
                pltpu.VMEM((2, 2, tok, half), jnp.float32),
                pltpu.VMEM((tok, 2 * half), bf),
                pltpu.VMEM((CORES, tok, hid), jnp.float32),
                pltpu.VMEM((CORES, tok, width), bf),
                pltpu.VMEM((chips, CORES, tok, 2 * half), bf),
                pltpu.VMEM((chips, tok, 2 * half), bf),
                pltpu.VMEM((CORES, tok, hid), bf),
                pltpu.VMEM((2, chips, 2, tok, half), bf),
                pltpu.VMEM((per_stage // CORES, ranks, tsh, 2 * half), bf),
                pltpu.VMEM((per_stage, chips, tsh, 2 * half), bf),
                dma((passes, 2)), dma((passes, 2)), dma((passes, 2)),
                dma, dma((chips,)), dma((visits,)), pltpu.SemaphoreType.REGULAR,
                dma((2,)), dma((visits,)), dma((3, 2)), dma((2,)), dma((visits, 2)), dma((visits,)), dma((visits,)), dma((2,)), dma((visits,)),
                dma((per_stage // CORES,)), dma((per_stage,)), dma, dma, dma, dma((chips,)),
            ],
            compiler_params=pltpu.CompilerParams(collective_id=0, has_side_effects=True, flags=FLAGS, vmem_limit_bytes=67043328),
        )(x, gain, w_in.reshape(passes, width, hid), w_out.reshape(passes, hid, width))

    return jax.shard_map(
        per_device,
        mesh=mesh,
        in_specs=(P("dp", "tp", None), P(None, "pp", None), P(None, "pp", None, "tp"), P(None, "pp", "tp", None)),
        out_specs=P(("dp", "pp"), "tp", None),
        check_vma=False,
    )
```

```python
import functools

import jax
import jax.numpy as jnp
from jax import lax
from jax.experimental import pallas as pl
from jax.experimental.pallas import tpu as pltpu
from jax.sharding import PartitionSpec as P

MESH = pl.DeviceIdType.MESH
NORM_EPS = 1e-5
CORES = 2
OWN_SHARE = 2
REDUCE_AT = 4
LEAD_AT = 5
LEADS = 1
FORWARD_AT = 10
LEAD_FWD = 10
FLAGS = {}
ADD_AT = 4
ADD_LEADS = 1
TILE = 256


def _f32(a):
    return a.astype(jnp.float32)


def _bf16(a):
    return a.astype(jnp.bfloat16)


def _kernel(dims, x_hbm, gain_ref, w1_hbm, w2_hbm, out_ref,
            w1, w2, xs, xbuf, ybuf, rbuf, stat, norm, lbuf, hold, hbuf, accb, hx, qbuf, qrecv, abuf, sbuf, tbuf, obuf,
            wl_sem, wp_send, wp_recv, xl_sem, x_send, x_recv, ready,
            rs_send, rs_recv, l_recv, ag_send, ag_first, ag_near, ag_far, st_send, st_recv, o_send, o_recv, h_send, h_recv, q_send, q_recv):
    stages, chips, visits, tok, width, hid = dims
    ranks = chips * CORES
    slab = width // chips
    half = slab // 2
    tsh = tok // ranks
    per_stage = visits * CORES // stages
    p = lax.axis_index("pp")
    t = lax.axis_index("tp")
    c = t // CORES
    k = lax.rem(t, CORES)
    nxt = lax.rem(p + 1, stages)
    right, left = lax.rem(c + 1, chips), lax.rem(c + chips - 1, chips)
    far = lax.rem(c + 2, chips)
    at_start = p == 0
    at_end = p == stages - 1

    def dev(pp, chip, core):
        return {"pp": pp, "tp": chip * CORES + core}

    def remote(src, dst, ssem, rsem, where):
        return pltpu.make_async_remote_copy(src_ref=src, dst_ref=dst, send_sem=ssem, recv_sem=rsem,
                                            device_id=where, device_id_type=MESH)

    def wait(ref, sem):
        pltpu.make_async_copy(ref, ref, sem).wait()

    def load_w(v, j):
        src, dst = ((w1_hbm, w1), (w2_hbm, w2))[j]
        return pltpu.make_async_copy(src.at[v], dst.at[v, k], wl_sem.at[v, j])

    def push_w(v, j):
        src, dst = ((w1_hbm, w1), (w2_hbm, w2))[j]
        return remote(src.at[v], dst.at[v, k], wp_send.at[v, j], wp_recv.at[v, j], dev(p, c, 1 - k))

    def push_piece(i):
        for j, (src, dst) in enumerate(((w1_hbm, w1), (w2_hbm, w2))):
            size = src.shape[1] // visits
            rows = pl.ds(pl.multiple_of(i * size, size), size)
            remote(src.at[1, rows], dst.at[1, k, rows], wp_send.at[1, j], wp_recv.at[1, j], dev(p, c, 1 - k)).start()

    x_load = pltpu.make_async_copy(x_hbm, xs, xl_sem)
    x_load.start()
    for v in range(2):
        for j in range(2):
            load_w(v, j).start()

    bar = pltpu.get_barrier_semaphore()
    for r in range(ranks):
        @pl.when(r != t)
        def _(r=r):
            pl.semaphore_signal(bar, inc=1, device_id={"pp": p, "tp": r}, device_id_type=MESH)

    @pl.when(jnp.logical_not(at_end))
    def _():
        for q in range(chips):
            pl.semaphore_signal(bar, inc=1, device_id=dev(nxt, q, k), device_id_type=MESH)

    @pl.when(at_start)
    def _():
        for r in range(ranks):
            pl.semaphore_signal(bar, inc=1, device_id={"pp": stages - 1, "tp": r}, device_id_type=MESH)
    known = jnp.where(at_start, ranks - 1, jnp.where(at_end, 2 * ranks - 1 + chips, ranks - 1 + chips))
    pl.semaphore_wait(bar, known)

    @pl.when(jnp.logical_not(at_start))
    def _():
        for q in range(chips):
            pl.semaphore_signal(ready, inc=1, device_id=dev(p - 1, q, k), device_id_type=MESH)

    def x_copy(i, core, chip):
        return remote(xs.at[CORES * i + core], xbuf.at[i, t], x_send.at[chip], x_recv.at[i], dev(0, chip, core))

    def x_share(i):
        for core in range(CORES):
            for chip in (far, right, left):
                x_copy(i, core, chip).start()

    @pl.when(at_start)
    def _():
        x_load.wait()
        for i in range(visits):
            x_copy(i, 1 - k, c).start()
        for i in range(OWN_SHARE):
            x_share(i)

    @pl.when(at_end)
    def _():
        x_load.wait()
        for i in range(OWN_SHARE, visits):
            x_share(i)

    @pl.when(jnp.logical_not(at_start))
    def _():
        for v in range(2):
            for j in range(2):
                push_w(v, j).start()

    def share(i, par, owner, h, chip, sem):
        return remote(ybuf.at[i, owner, h], ybuf.at[i, owner, h], ag_send.at[par], sem, dev(p, chip, k))

    def reduce_slab(idx):
        i = lax.rem(idx, visits)
        par = lax.rem(idx, 2)

        @pl.when(idx >= jnp.where(at_start, visits + 2, 2))
        def _():
            wait(ybuf.at[i, 0:3], ag_send.at[par])
            wait(stat.at[i, 0:3], st_send.at[par])

        with jax.named_scope("wait_rs"):
            wait(rbuf.at[i], rs_recv.at[i])
        own = [_bf16(_f32(rbuf[i, 0, h]) + _f32(rbuf[i, 1, h]) + _f32(rbuf[i, 2, h])) for h in range(2)]
        for h in range(2):
            ybuf[i, c, h] = own[h]
        share(i, par, c, 0, right, ag_first.at[i, 0]).start()
        share(i, par, c, 1, left, ag_first.at[i, 1]).start()
        own = [_f32(a) for a in own]
        mean = sum(jnp.sum(a, axis=-1, keepdims=True) for a in own) * (1.0 / slab)
        dev2 = sum(jnp.sum((a - mean) * (a - mean), axis=-1, keepdims=True) for a in own)
        lane = lax.broadcasted_iota(jnp.int32, (8, 128), 1)
        tile = jnp.zeros((8, 128), jnp.float32)
        for j, col in enumerate((mean, dev2)):
            for a in range(tok // 8):
                tile = jnp.where(lane == tok // 8 * j + a, col[8 * a:8 * a + 8, :], tile)
        stat[i, c] = tile
        for chip in (far, right, left):
            remote(stat.at[i, c], stat.at[i, c], st_send.at[par], st_recv.at[i], dev(p, chip, k)).start()
        share(i, par, c, 1, right, ag_near.at[i]).start()
        share(i, par, c, 0, left, ag_near.at[i]).start()

    def forward(idx):
        i = lax.rem(idx, visits)
        par = lax.rem(idx, 2)
        with jax.named_scope("wait_fwd"):
            wait(ybuf.at[i, left, 0], ag_first.at[i, 0])
            share(i, par, left, 0, right, ag_far.at[i]).start()
            wait(ybuf.at[i, right, 1], ag_first.at[i, 1])
            share(i, par, right, 1, left, ag_far.at[i]).start()

    @pl.when(jnp.logical_not(at_start))
    def _():
        reduce_slab(0)
        forward(0)

    def add_relayed(idx):
        i = lax.rem(idx, visits)
        par = lax.rem(idx, 2)
        dst = jnp.where(at_end & (idx >= visits), CORES * i // per_stage, nxt)
        for slot, chip, h in ((1, right, 0), (2, left, 1)):
            got = lax.rem(idx, 3)
            with jax.named_scope("wait_l"):
                wait(lbuf.at[got, h], l_recv.at[got, h])
            sbuf[par, slot, h] = _bf16(hold[par, h] + _f32(lbuf[got, h]))
            remote(sbuf.at[par, slot, h], rbuf.at[i, slot, h], rs_send.at[par], rs_recv.at[i], dev(dst, chip, k)).start()

    def visit(kind, idx, carry):
        v = 0 if kind == "first" else idx // visits
        i = lax.rem(idx, visits)
        dst = jnp.where(at_end & (v == 1), CORES * i // per_stage, nxt)
        par = lax.rem(idx, 2)

        def at(place):
            if place == ADD_AT and place < 10:
                @pl.when(i > ADD_LEADS)
                def _():
                    add_relayed(idx - 1)
            if kind == "first":
                return
            ahead = (idx + 1 < 2 * visits) & (idx + 1 != visits)
            if place == REDUCE_AT:
                @pl.when(ahead & (i >= LEADS))
                def _():
                    reduce_slab(idx + 1)
            if place == LEAD_AT:
                @pl.when(ahead & (i < LEADS))
                def _():
                    reduce_slab(idx + 1)
            if place == LEAD_FWD and LEAD_FWD < 11:
                @pl.when(ahead & (i < LEADS))
                def _():
                    forward(idx + 1)
            if place == FORWARD_AT:
                @pl.when(ahead & (i >= LEADS))
                def _():
                    forward(idx + 1)

        if kind == "first":
            xbuf[i, t] = xs[CORES * i + k]
            with jax.named_scope("wait_x"):
                wait(xbuf.at[i, 0:ranks - 1], x_recv.at[i])
            for q in range(chips):
                for h in range(2):
                    lo = q * slab + h * half
                    ybuf[i, q, h] = _bf16(_f32(xbuf[i, :, :, lo:lo + half]).reshape(tok, half))

        at(1)

        def keep(mean, scale):
            norm[0] = jnp.broadcast_to(mean, (tok, 128))
            norm[1] = jnp.broadcast_to(scale, (tok, 128))

        if kind == "first":
            pieces = [(q, h) for q in range(chips) for h in range(2)]
            mean = sum(jnp.sum(_f32(ybuf[i, q, h]), axis=-1, keepdims=True) for q, h in pieces) * (1.0 / width)
            var = jnp.zeros_like(mean)
            for q, h in pieces:
                a = _f32(ybuf[i, q, h]) - mean
                var = var + jnp.sum(a * a, axis=-1, keepdims=True)
            keep(mean, lax.rsqrt(var * (1.0 / width) + NORM_EPS))

        else:
            with jax.named_scope("wait_st"):
                wait(stat.at[i, 0:3], st_recv.at[i])
            groups = tok // 8
            means = [stat[i, q][:, :groups] for q in range(chips)]
            devs = [stat[i, q][:, groups:2 * groups] for q in range(chips)]
            mean = sum(means) * (1.0 / chips)
            dev2 = sum(devs[q] + slab * (means[q] - mean) * (means[q] - mean) for q in range(chips))
            scale = lax.rsqrt(dev2 * (1.0 / width) + NORM_EPS)
            for a in range(groups):
                rows = slice(8 * a, 8 * a + 8)
                norm[0, rows] = jnp.broadcast_to(mean[:, a:a + 1], (8, 128))
                norm[1, rows] = jnp.broadcast_to(scale[:, a:a + 1], (8, 128))

        def wait_weights(j):
            @pl.when(i == 0)
            def _():
                load_w(v, j).wait()
                if kind != "first":
                    push_w(v, j).wait_recv()

        with jax.named_scope("wait_w1"):
            wait_weights(0)
        at(2)
        tile = TILE
        if kind == "first":
            @pl.when(i > 0)
            def _():
                wait(hx.at[0], h_send)
            for q in range(chips):
                for m in range(slab // 128):
                    cols = slice(q * slab + m * 128, q * slab + (m + 1) * 128)
                    h, lo = m * 128 // half, m * 128 % half
                    hx[k, :, cols] = _bf16((_f32(ybuf[i, q, h, :, lo:lo + 128]) - norm[0]) * norm[1] * _f32(gain_ref[v, :, cols]))
            remote(hx.at[k], hx.at[k], h_send, h_recv, dev(p, c, 1 - k)).start()

            @pl.when(i > 0)
            def _():
                add_relayed(idx - 1)
            with jax.named_scope("wait_h"):
                wait(hx.at[0], h_recv)
            for col in range(0, hid, 2 * tile):
                cols = slice(col, col + 2 * tile)
                part = jnp.dot(hx[...].reshape(CORES * tok, width), w1[v, k, :, cols], preferred_element_type=jnp.float32)
                abuf[:, :, cols] = _bf16(jax.nn.gelu(part)).reshape(CORES, tok, 2 * tile)
        for n_done, chip in enumerate((c, right, left, far) if kind != "first" else ()):
            if n_done in (1, 3):
                with jax.named_scope("wait_ag"):
                    wait(ybuf.at[i, 0], (None, ag_near, None, ag_far)[n_done].at[i])
            for m in range(slab // 128):
                cols = slice(m * 128, (m + 1) * 128)
                gain = gain_ref[v, :, pl.ds(pl.multiple_of(chip * slab + m * 128, 128), 128)]
                h, lo = m * 128 // half, m * 128 % half
                hbuf[:, cols] = _bf16((_f32(ybuf[i, chip, h, :, lo:lo + 128]) - norm[0]) * norm[1] * _f32(gain))
            for s in range(CORES):
                for col in range(0, hid, 2 * tile):
                    rows = pl.ds(pl.multiple_of(chip * slab, slab), slab)
                    cols = slice(col, col + 2 * tile)
                    part = jnp.dot(hbuf[...], w1[v, s, rows, cols], preferred_element_type=jnp.float32)
                    if n_done:
                        part = part + accb[s, :, cols]
                    if n_done < 3:
                        accb[s, :, cols] = part
                    else:
                        abuf[s, :, cols] = _bf16(jax.nn.gelu(part))
            if n_done < 3:
                at(3 + n_done)
        at(6)
        with jax.named_scope("wait_w2"):
            wait_weights(1)

        @pl.when(idx == 0)
        def _():
            @pl.when(jnp.logical_not(at_end))
            def _():
                pl.semaphore_wait(ready, chips)

        @pl.when(idx >= 2)
        def _():
            wait(sbuf.at[par], rs_send.at[par])

        def partial(slot, h, dst, where, sem):
            return remote(sbuf.at[par, slot, h], dst, rs_send.at[par], sem, where)

        def slab_done(n, q, prod):
            prod = prod[:, :half], prod[:, half:]
            if n == 0:
                got = lax.rem(idx, 3)
                for h, chip in ((0, right), (1, left)):
                    sbuf[par, 0, h] = _bf16(prod[h])
                    partial(0, h, lbuf.at[got, h], dev(p, chip, k), l_recv.at[got, h]).start()
            elif n == 3:
                for h in range(2):
                    sbuf[par, 3, h] = _bf16(prod[h] + _f32(ybuf[i, c, h]))


                @pl.when(dst != p)
                def _():
                    remote(sbuf.at[par, 3], rbuf.at[i, 0], rs_send.at[par], rs_recv.at[i], dev(dst, c, k)).start()

                @pl.when(dst == p)
                def _():
                    rbuf[i, 0] = sbuf[par, 3]
            else:
                h = 2 - n
                sbuf[par, n, h] = _bf16(prod[h])
                hold[par, 1 - h] = prod[1 - h]
                partial(n, h, rbuf.at[i, n, h], dev(dst, q, k), rs_recv.at[i]).start()

        order = (far, right, left, c)
        if kind == "first":
            @pl.when(i > 0)
            def _():
                wait(qrecv, q_send)
            for n, q in enumerate(order):
                cols = pl.ds(pl.multiple_of(q * slab, slab), slab)
                prod = jnp.dot(abuf[...].reshape(CORES * tok, hid), w2[v, k, :, cols], preferred_element_type=jnp.float32)
                qbuf[n] = _bf16(prod).reshape(CORES, tok, slab)
                remote(qbuf.at[n, 1 - k], qrecv.at[n], q_send, q_recv.at[n], dev(p, c, 1 - k)).start()
            for n, q in enumerate(order):
                with jax.named_scope("wait_q"):
                    wait(qrecv.at[n], q_recv.at[n])
                slab_done(n, q, _f32(qbuf[n, k]) + _f32(qrecv[n]))
            push_piece(i)
        for n, q in enumerate(order if kind != "first" else ()):
            cols = pl.ds(pl.multiple_of(q * slab, slab), slab)
            prod = jnp.zeros((tok, slab), jnp.float32)
            for s in range(CORES):
                prod = prod + _f32(_bf16(jnp.dot(abuf[s], w2[v, s, :, cols], preferred_element_type=jnp.float32)))
            slab_done(n, q, prod)
            if n < 3:
                at(7 + n)
        at(10)
        @pl.when((i == visits - 1) if kind == "first" else (i < ADD_LEADS) | (i == visits - 1) | (ADD_AT > 9))
        def _():
            add_relayed(idx)
        at(11)
        if kind == "mid":
            @pl.when((LEAD_FWD > 10) & (i < LEADS) & (idx + 1 < 2 * visits) & (idx + 1 != visits))
            def _():
                forward(idx + 1)

        @pl.when(idx + 1 == visits)
        def _():
            reduce_slab(idx + 1)
            forward(idx + 1)

        return carry

    mid_from = jnp.where(at_start, visits, 0)
    lax.fori_loop(0, mid_from, functools.partial(visit, "first"), 0)
    lax.fori_loop(mid_from, 2 * visits, functools.partial(visit, "mid"), 0)

    per_core = per_stage // CORES
    with jax.named_scope("wait_out"):
        for n in range(per_core):
            i = per_core * p + n
            j = CORES * n + k

            @pl.when(at_end)
            def _(i=i):
                wait(rbuf.at[i, 0:2], rs_recv.at[i])

            @pl.when(jnp.logical_not(at_end))
            def _(i=i):
                wait(rbuf.at[i], rs_recv.at[i])
            for h in range(2):
                total = _bf16(_f32(rbuf[i, 0, h]) + _f32(rbuf[i, 1, h]) + _f32(rbuf[i, 2, h]))
                tbuf[n, :, :, h * half:(h + 1) * half] = _bf16(_f32(total).reshape(ranks, tsh, half))
            for r in range(ranks):
                @pl.when(r == t)
                def _(r=r, n=n, j=j):
                    obuf[j, c] = tbuf[n, r]

                @pl.when(r != t)
                def _(r=r, n=n, j=j):
                    remote(tbuf.at[n, r], obuf.at[j, c], o_send.at[n], o_recv.at[j], {"pp": p, "tp": r}).start()
    with jax.named_scope("wait_out2"):
        for j in range(per_stage):
            @pl.when(j % CORES == k)
            def _(j=j):
                wait(obuf.at[j, 0:chips - 1], o_recv.at[j])

            @pl.when(j % CORES != k)
            def _(j=j):
                wait(obuf.at[j], o_recv.at[j])
            for q in range(chips):
                out_ref[j, :, q * slab:(q + 1) * slab] = obuf[j, q]

    with jax.named_scope("wait_sends"):
        @pl.when(at_start)
        def _():
            wait(hx.at[0], h_send)
            wait(qrecv, q_send)
        for n in range(per_core):
            wait(tbuf.at[n, 0:ranks - 1], o_send.at[n])
        for par in range(2):
            @pl.when(at_end)
            def _(par=par):
                wait(sbuf.at[par, 0:3], rs_send.at[par])

            @pl.when(jnp.logical_not(at_end))
            def _(par=par):
                wait(sbuf.at[par], rs_send.at[par])
            wait(ybuf.at[0, 0:3], ag_send.at[par])
            wait(stat.at[0, 0:3], st_send.at[par])
        for v in range(2):
            @pl.when((v == 1) | jnp.logical_not(at_start))
            def _(v=v):
                for j in range(2):
                    push_w(v, j).wait_send()

        @pl.when(jnp.logical_not(at_start | at_end))
        def _():
            x_load.wait()

        @pl.when(at_start)
        def _():
            wait(xs.at[0:visits], x_send.at[c])
            for chip in (far, right, left):
                wait(xs.at[0:CORES * OWN_SHARE], x_send.at[chip])

        @pl.when(at_end)
        def _():
            for chip in (far, right, left):
                wait(xs.at[0:CORES * (visits - OWN_SHARE)], x_send.at[chip])


def solution(mesh):
    stages, ranks = mesh.shape["pp"], mesh.shape["tp"]
    chips = ranks // CORES

    def per_device(x, gain, w_in, w_out):
        micro, tsh, width = x.shape
        passes, _, _, hid = w_in.shape
        tok = tsh * ranks
        visits = micro // CORES
        half = width // chips // 2
        per_stage = micro // stages
        dims = (stages, chips, visits, tok, width, hid)
        bf = jnp.bfloat16
        dma = pltpu.SemaphoreType.DMA
        any_space = pl.BlockSpec(memory_space=pl.ANY)
        vmem = pl.BlockSpec(memory_space=pltpu.VMEM)
        return pl.pallas_call(
            functools.partial(_kernel, dims),
            name="mlp_pipe",
            out_shape=jax.ShapeDtypeStruct((per_stage, tsh, width), bf),
            in_specs=[any_space, vmem, any_space, any_space],
            out_specs=vmem,
            scratch_shapes=[
                pltpu.VMEM((passes, CORES, width, hid), bf),
                pltpu.VMEM((passes, CORES, hid, width), bf),
                pltpu.VMEM((micro, tsh, width), bf),
                pltpu.VMEM((visits, ranks, tsh, width), bf),
                pltpu.VMEM((visits, chips, 2, tok, half), bf),
                pltpu.VMEM((visits, 3, 2, tok, half), bf),
                pltpu.VMEM((visits, chips, 8, 128), jnp.float32),
                pltpu.VMEM((2, tok, 128), jnp.float32),
                pltpu.VMEM((3, 2, tok, half), bf),
                pltpu.VMEM((2, 2, tok, half), jnp.float32),
                pltpu.VMEM((tok, 2 * half), bf),
                pltpu.VMEM((CORES, tok, hid), jnp.float32),
                pltpu.VMEM((CORES, tok, width), bf),
                pltpu.VMEM((chips, CORES, tok, 2 * half), bf),
                pltpu.VMEM((chips, tok, 2 * half), bf),
                pltpu.VMEM((CORES, tok, hid), bf),
                pltpu.VMEM((2, chips, 2, tok, half), bf),
                pltpu.VMEM((per_stage // CORES, ranks, tsh, 2 * half), bf),
                pltpu.VMEM((per_stage, chips, tsh, 2 * half), bf),
                dma((passes, 2)), dma((passes, 2)), dma((passes, 2)),
                dma, dma((chips,)), dma((visits,)), pltpu.SemaphoreType.REGULAR,
                dma((2,)), dma((visits,)), dma((3, 2)), dma((2,)), dma((visits, 2)), dma((visits,)), dma((visits,)), dma((2,)), dma((visits,)),
                dma((per_stage // CORES,)), dma((per_stage,)), dma, dma, dma, dma((chips,)),
            ],
            compiler_params=pltpu.CompilerParams(collective_id=0, has_side_effects=True, flags=FLAGS, vmem_limit_bytes=67043328),
        )(x, gain, w_in.reshape(passes, width, hid), w_out.reshape(passes, hid, width))

    return jax.shard_map(
        per_device,
        mesh=mesh,
        in_specs=(P("dp", "tp", None), P(None, "pp", None), P(None, "pp", None, "tp"), P(None, "pp", "tp", None)),
        out_specs=P(("dp", "pp"), "tp", None),
        check_vma=False,
    )
```

```python
import functools

import jax
import jax.numpy as jnp
from jax import lax
from jax.experimental import pallas as pl
from jax.experimental.pallas import tpu as pltpu
from jax.sharding import PartitionSpec as P

MESH = pl.DeviceIdType.MESH
NORM_EPS = 1e-5
CORES = 2
OWN_SHARE = 2
ORDER = (0, 1, 2, 3)
FIRST_ORDER = (3, 0, 1, 2)
REDUCE_AT = 4
LEAD_AT = 5
LEADS = 1
FORWARD_AT = 10
LEAD_FWD = 10
FLAGS = {}
ADD_AT = 4
ADD_LEADS = 2
TILE = 256


def _f32(a):
    return a.astype(jnp.float32)


def _bf16(a):
    return a.astype(jnp.bfloat16)


def _kernel(dims, x_hbm, gain_ref, w1_hbm, w2_hbm, out_ref,
            w1, w2, xs, xbuf, ybuf, rbuf, stat, norm, lbuf, hold, hbuf, accb, hx, qbuf, qrecv, abuf, sbuf, tbuf, obuf, fbuf, gbuf,
            wl_sem, wp_send, wp_recv, xl_sem, x_send, x_recv, ready,
            rs_send, rs_recv, l_recv, ag_send, ag_first, ag_near, ag_far, st_send, st_recv, o_send, o_recv, h_send, h_recv, q_send, q_recv, g_send, g_recv):
    stages, chips, visits, tok, width, hid = dims
    ranks = chips * CORES
    slab = width // chips
    half = slab // 2
    tsh = tok // ranks
    per_stage = visits * CORES // stages
    p = lax.axis_index("pp")
    t = lax.axis_index("tp")
    c = t // CORES
    k = lax.rem(t, CORES)
    nxt = lax.rem(p + 1, stages)
    right, left = lax.rem(c + 1, chips), lax.rem(c + chips - 1, chips)
    far = lax.rem(c + 2, chips)
    at_start = p == 0
    at_end = p == stages - 1

    def dev(pp, chip, core):
        return {"pp": pp, "tp": chip * CORES + core}

    def remote(src, dst, ssem, rsem, where):
        return pltpu.make_async_remote_copy(src_ref=src, dst_ref=dst, send_sem=ssem, recv_sem=rsem,
                                            device_id=where, device_id_type=MESH)

    def wait(ref, sem):
        pltpu.make_async_copy(ref, ref, sem).wait()

    def load_w(v, j):
        src, dst = ((w1_hbm, w1), (w2_hbm, w2))[j]
        return pltpu.make_async_copy(src.at[v], dst.at[v, k], wl_sem.at[v, j])

    def push_w(v, j):
        src, dst = ((w1_hbm, w1), (w2_hbm, w2))[j]
        return remote(src.at[v], dst.at[v, k], wp_send.at[v, j], wp_recv.at[v, j], dev(p, c, 1 - k))

    def push_piece(i):
        for j, (src, dst) in enumerate(((w1_hbm, w1), (w2_hbm, w2))):
            size = src.shape[1] // visits
            rows = pl.ds(pl.multiple_of(i * size, size), size)
            remote(src.at[1, rows], dst.at[1, k, rows], wp_send.at[1, j], wp_recv.at[1, j], dev(p, c, 1 - k)).start()

    x_load = pltpu.make_async_copy(x_hbm, xs, xl_sem)
    x_load.start()
    for v in range(2):
        for j in range(2):
            load_w(v, j).start()

    bar = pltpu.get_barrier_semaphore()
    for r in range(ranks):
        @pl.when(r != t)
        def _(r=r):
            pl.semaphore_signal(bar, inc=1, device_id={"pp": p, "tp": r}, device_id_type=MESH)

    @pl.when(jnp.logical_not(at_end))
    def _():
        for q in range(chips):
            pl.semaphore_signal(bar, inc=1, device_id=dev(nxt, q, k), device_id_type=MESH)

    @pl.when(at_start)
    def _():
        for r in range(ranks):
            pl.semaphore_signal(bar, inc=1, device_id={"pp": stages - 1, "tp": r}, device_id_type=MESH)
    known = jnp.where(at_start, ranks - 1, jnp.where(at_end, 2 * ranks - 1 + chips, ranks - 1 + chips))
    pl.semaphore_wait(bar, known)

    @pl.when(jnp.logical_not(at_start))
    def _():
        for q in range(chips):
            pl.semaphore_signal(ready, inc=1, device_id=dev(p - 1, q, k), device_id_type=MESH)

    def x_copy(i, core, chip):
        return remote(xs.at[CORES * i + core], xbuf.at[i, t], x_send.at[chip], x_recv.at[i], dev(0, chip, core))

    def x_share(i):
        for core in range(CORES):
            for chip in (far, right, left):
                x_copy(i, core, chip).start()

    @pl.when(at_start)
    def _():
        x_load.wait()
        for i in range(visits):
            x_copy(i, 1 - k, c).start()
        for i in range(OWN_SHARE):
            x_share(i)

    @pl.when(at_end)
    def _():
        x_load.wait()
        for i in range(OWN_SHARE, visits):
            x_share(i)

    @pl.when(jnp.logical_not(at_start))
    def _():
        for v in range(2):
            for j in range(2):
                push_w(v, j).start()

    def share(i, par, owner, h, chip, sem):
        return remote(ybuf.at[i, owner, h], ybuf.at[i, owner, h], ag_send.at[par], sem, dev(p, chip, k))

    def reduce_slab(idx):
        i = lax.rem(idx, visits)
        par = lax.rem(idx, 2)

        @pl.when(idx >= jnp.where(at_start, visits + 2, 2))
        def _():
            wait(ybuf.at[i, 0:3], ag_send.at[par])
            wait(stat.at[i, 0:3], st_send.at[par])

        with jax.named_scope("wait_rs"):
            wait(rbuf.at[i], rs_recv.at[i])
        own = [_bf16(_f32(rbuf[i, 0, h]) + _f32(rbuf[i, 1, h]) + _f32(rbuf[i, 2, h])) for h in range(2)]
        for h in range(2):
            ybuf[i, c, h] = own[h]
        share(i, par, c, 0, right, ag_first.at[i, 0]).start()
        share(i, par, c, 1, left, ag_first.at[i, 1]).start()
        own = [_f32(a) for a in own]
        mean = sum(jnp.sum(a, axis=-1, keepdims=True) for a in own) * (1.0 / slab)
        dev2 = sum(jnp.sum((a - mean) * (a - mean), axis=-1, keepdims=True) for a in own)
        lane = lax.broadcasted_iota(jnp.int32, (8, 128), 1)
        tile = jnp.zeros((8, 128), jnp.float32)
        for j, col in enumerate((mean, dev2)):
            for a in range(tok // 8):
                tile = jnp.where(lane == tok // 8 * j + a, col[8 * a:8 * a + 8, :], tile)
        stat[i, c] = tile
        for chip in (far, right, left):
            remote(stat.at[i, c], stat.at[i, c], st_send.at[par], st_recv.at[i], dev(p, chip, k)).start()
        share(i, par, c, 1, right, ag_near.at[i]).start()
        share(i, par, c, 0, left, ag_near.at[i]).start()

    def forward(idx):
        i = lax.rem(idx, visits)
        par = lax.rem(idx, 2)
        with jax.named_scope("wait_fwd"):
            wait(ybuf.at[i, left, 0], ag_first.at[i, 0])
            share(i, par, left, 0, right, ag_far.at[i]).start()
            wait(ybuf.at[i, right, 1], ag_first.at[i, 1])
            share(i, par, right, 1, left, ag_far.at[i]).start()

    @pl.when(jnp.logical_not(at_start))
    def _():
        reduce_slab(0)
        forward(0)

    def add_relayed(idx):
        i = lax.rem(idx, visits)
        par = lax.rem(idx, 2)
        dst = jnp.where(at_end & (idx >= visits), CORES * i // per_stage, nxt)
        for slot, chip, h in ((1, right, 0), (2, left, 1)):
            got = lax.rem(idx, 3)
            with jax.named_scope("wait_l"):
                wait(lbuf.at[got, h], l_recv.at[got, h])
            sbuf[par, slot, h] = _bf16(hold[par, h] + _f32(lbuf[got, h]))
            remote(sbuf.at[par, slot, h], rbuf.at[i, slot, h], rs_send.at[par], rs_recv.at[i], dev(dst, chip, k)).start()

    def visit(kind, idx, carry):
        v = 0 if kind == "first" else idx // visits
        i = lax.rem(idx, visits)
        dst = jnp.where(at_end & (v == 1), CORES * i // per_stage, nxt)
        par = lax.rem(idx, 2)

        def at(place):
            if kind == "last":
                if place == ADD_AT and place < 10:
                    add_relayed(idx - 1)
                return
            if place == ADD_AT and place < 10:
                @pl.when(i > ADD_LEADS)
                def _():
                    add_relayed(idx - 1)
            if kind == "first":
                return
            ahead = (idx + 1 < 2 * visits) & (idx + 1 != visits)
            if place == REDUCE_AT:
                @pl.when(ahead & (i >= LEADS))
                def _():
                    reduce_slab(idx + 1)
            if place == LEAD_AT:
                @pl.when(ahead & (i < LEADS))
                def _():
                    reduce_slab(idx + 1)
            if place == LEAD_FWD and LEAD_FWD < 11:
                @pl.when(ahead & (i < LEADS))
                def _():
                    forward(idx + 1)
            if place == FORWARD_AT:
                @pl.when(ahead & (i >= LEADS))
                def _():
                    forward(idx + 1)

        if kind == "first":
            xbuf[i, t] = xs[CORES * i + k]
            with jax.named_scope("wait_x"):
                wait(xbuf.at[i, 0:ranks - 1], x_recv.at[i])
            for q in range(chips):
                for h in range(2):
                    lo = q * slab + h * half
                    ybuf[i, q, h] = _bf16(_f32(xbuf[i, :, :, lo:lo + half]).reshape(tok, half))

        at(1)

        def keep(mean, scale):
            norm[0] = jnp.broadcast_to(mean, (tok, 128))
            norm[1] = jnp.broadcast_to(scale, (tok, 128))

        if kind == "first":
            pieces = [(q, h) for q in range(chips) for h in range(2)]
            mean = sum(jnp.sum(_f32(ybuf[i, q, h]), axis=-1, keepdims=True) for q, h in pieces) * (1.0 / width)
            var = jnp.zeros_like(mean)
            for q, h in pieces:
                a = _f32(ybuf[i, q, h]) - mean
                var = var + jnp.sum(a * a, axis=-1, keepdims=True)
            keep(mean, lax.rsqrt(var * (1.0 / width) + NORM_EPS))

        else:
            with jax.named_scope("wait_st"):
                wait(stat.at[i, 0:3], st_recv.at[i])
            groups = tok // 8
            means = [stat[i, q][:, :groups] for q in range(chips)]
            devs = [stat[i, q][:, groups:2 * groups] for q in range(chips)]
            mean = sum(means) * (1.0 / chips)
            dev2 = sum(devs[q] + slab * (means[q] - mean) * (means[q] - mean) for q in range(chips))
            scale = lax.rsqrt(dev2 * (1.0 / width) + NORM_EPS)
            for a in range(groups):
                rows = slice(8 * a, 8 * a + 8)
                norm[0, rows] = jnp.broadcast_to(mean[:, a:a + 1], (8, 128))
                norm[1, rows] = jnp.broadcast_to(scale[:, a:a + 1], (8, 128))

        def wait_weights(j):
            @pl.when(i == 0)
            def _():
                load_w(v, j).wait()
                if kind != "first":
                    push_w(v, j).wait_recv()

        with jax.named_scope("wait_w1"):
            wait_weights(0)
        at(2)
        tile = TILE
        if kind == "first":
            @pl.when(i > 0)
            def _():
                wait(hx.at[0], h_send)
            for q in range(chips):
                for m in range(slab // 128):
                    cols = slice(q * slab + m * 128, q * slab + (m + 1) * 128)
                    h, lo = m * 128 // half, m * 128 % half
                    hx[k, :, cols] = _bf16((_f32(ybuf[i, q, h, :, lo:lo + 128]) - norm[0]) * norm[1] * _f32(gain_ref[v, :, cols]))
            remote(hx.at[k], hx.at[k], h_send, h_recv, dev(p, c, 1 - k)).start()

            @pl.when(i > 0)
            def _():
                add_relayed(idx - 1)
            with jax.named_scope("wait_h"):
                wait(hx.at[0], h_recv)
            for col in range(0, hid, 2 * tile):
                cols = slice(col, col + 2 * tile)
                part = jnp.dot(hx[...].reshape(CORES * tok, width), w1[v, k, :, cols], preferred_element_type=jnp.float32)
                abuf[:, :, cols] = _bf16(jax.nn.gelu(part)).reshape(CORES, tok, 2 * tile)
        for n_done, chip in enumerate((c, right, left, far) if kind != "first" else ()):
            if n_done in (1, 3):
                with jax.named_scope("wait_ag"):
                    wait(ybuf.at[i, 0], (None, ag_near, None, ag_far)[n_done].at[i])
            for m in range(slab // 128):
                cols = slice(m * 128, (m + 1) * 128)
                gain = gain_ref[v, :, pl.ds(pl.multiple_of(chip * slab + m * 128, 128), 128)]
                h, lo = m * 128 // half, m * 128 % half
                hbuf[:, cols] = _bf16((_f32(ybuf[i, chip, h, :, lo:lo + 128]) - norm[0]) * norm[1] * _f32(gain))
            for s in range(CORES):
                for col in range(0, hid, 2 * tile):
                    rows = pl.ds(pl.multiple_of(chip * slab, slab), slab)
                    cols = slice(col, col + 2 * tile)
                    part = jnp.dot(hbuf[...], w1[v, s, rows, cols], preferred_element_type=jnp.float32)
                    if n_done:
                        part = part + accb[s, :, cols]
                    if n_done < 3:
                        accb[s, :, cols] = part
                    else:
                        abuf[s, :, cols] = _bf16(jax.nn.gelu(part))
            if n_done < 3:
                at(3 + n_done)
        at(6)
        with jax.named_scope("wait_w2"):
            wait_weights(1)

        @pl.when(idx == 0)
        def _():
            @pl.when(jnp.logical_not(at_end))
            def _():
                pl.semaphore_wait(ready, chips)

        @pl.when(idx >= 2)
        def _():
            wait(sbuf.at[par], rs_send.at[par])

        def partial(slot, h, dst, where, sem):
            return remote(sbuf.at[par, slot, h], dst, rs_send.at[par], sem, where)

        row_chip = lax.broadcasted_iota(jnp.int32, (tok, slab), 0) // (tsh * CORES)

        def tokens_done(n, q, prod):
            whole = jnp.concatenate([_f32(ybuf[i, q, 0]), _f32(ybuf[i, q, 1])], axis=1)
            fbuf[n] = _bf16((prod + jnp.where(row_chip == c, whole, 0.0)).reshape(ranks, tsh, slab))
            for r in range(ranks):
                @pl.when(r == t)
                def _(r=r):
                    gbuf[k, c, q] = fbuf[n, r]

                @pl.when(r != t)
                def _(r=r):
                    remote(fbuf.at[n, r], gbuf.at[k, c, q], g_send, g_recv.at[k], {"pp": p, "tp": r}).start()

        def slab_done(n, q, prod):
            if kind == "last":
                return tokens_done(n, q, prod)
            prod = prod[:, :half], prod[:, half:]
            if n == 0:
                got = lax.rem(idx, 3)
                for h, chip in ((0, right), (1, left)):
                    sbuf[par, 0, h] = _bf16(prod[h])
                    partial(0, h, lbuf.at[got, h], dev(p, chip, k), l_recv.at[got, h]).start()
            elif n == 3:
                for h in range(2):
                    sbuf[par, 3, h] = _bf16(prod[h] + _f32(ybuf[i, c, h]))


                @pl.when(dst != p)
                def _():
                    remote(sbuf.at[par, 3], rbuf.at[i, 0], rs_send.at[par], rs_recv.at[i], dev(dst, c, k)).start()

                @pl.when(dst == p)
                def _():
                    rbuf[i, 0] = sbuf[par, 3]
            else:
                h = 2 - n
                sbuf[par, n, h] = _bf16(prod[h])
                hold[par, 1 - h] = prod[1 - h]
                partial(n, h, rbuf.at[i, n, h], dev(dst, q, k), rs_recv.at[i]).start()

        order = (far, right, left, c)
        if kind == "first":
            @pl.when(i > 0)
            def _():
                wait(qrecv, q_send)
            for n in FIRST_ORDER:
                q = order[n]
                cols = pl.ds(pl.multiple_of(q * slab, slab), slab)
                prod = jnp.dot(abuf[...].reshape(CORES * tok, hid), w2[v, k, :, cols], preferred_element_type=jnp.float32)
                qbuf[n] = _bf16(prod).reshape(CORES, tok, slab)
                remote(qbuf.at[n, 1 - k], qrecv.at[n], q_send, q_recv.at[n], dev(p, c, 1 - k)).start()
            for n in FIRST_ORDER:
                q = order[n]
                with jax.named_scope("wait_q"):
                    wait(qrecv.at[n], q_recv.at[n])
                slab_done(n, q, _f32(qbuf[n, k]) + _f32(qrecv[n]))
            push_piece(i)
        for m, n in enumerate(ORDER if kind != "first" else ()):
            q = order[n]
            cols = pl.ds(pl.multiple_of(q * slab, slab), slab)
            prod = jnp.zeros((tok, slab), jnp.float32)
            for s in range(CORES):
                prod = prod + _f32(_bf16(jnp.dot(abuf[s], w2[v, s, :, cols], preferred_element_type=jnp.float32)))
            slab_done(n, q, prod)
            if m < 3:
                at(7 + m)
        at(10)
        if kind == "last":
            return carry

        @pl.when((i == visits - 1) if kind == "first" else (i < ADD_LEADS) | (i == visits - 1) | (ADD_AT > 9))
        def _():
            add_relayed(idx)
        at(11)
        if kind == "mid":
            @pl.when((LEAD_FWD > 10) & (i < LEADS) & (idx + 1 < 2 * visits) & (idx + 1 != visits))
            def _():
                forward(idx + 1)

        @pl.when(idx + 1 == visits)
        def _():
            reduce_slab(idx + 1)
            forward(idx + 1)

        return carry

    mid_from = jnp.where(at_start, visits, 0)
    lax.fori_loop(0, mid_from, functools.partial(visit, "first"), 0)
    lax.fori_loop(mid_from, 2 * visits - jnp.where(at_end, 1, 0), functools.partial(visit, "mid"), 0)

    @pl.when(at_end)
    def _():
        visit("last", 2 * visits - 1, 0)

    per_core = per_stage // CORES
    with jax.named_scope("wait_out"):
        for n in range(per_core):
            i = per_core * p + n
            j = CORES * n + k

            @pl.when(jnp.logical_not(at_end & (n == per_core - 1)))
            def _(n=n, i=i, j=j):
                @pl.when(at_end)
                def _(i=i):
                    wait(rbuf.at[i, 0:2], rs_recv.at[i])

                @pl.when(jnp.logical_not(at_end))
                def _(i=i):
                    wait(rbuf.at[i], rs_recv.at[i])
                for h in range(2):
                    total = _bf16(_f32(rbuf[i, 0, h]) + _f32(rbuf[i, 1, h]) + _f32(rbuf[i, 2, h]))
                    tbuf[n, :, :, h * half:(h + 1) * half] = _bf16(_f32(total).reshape(ranks, tsh, half))
                for r in range(ranks):
                    @pl.when(r == t)
                    def _(r=r, n=n, j=j):
                        obuf[j, c] = tbuf[n, r]

                    @pl.when(r != t)
                    def _(r=r, n=n, j=j):
                        remote(tbuf.at[n, r], obuf.at[j, c], o_send.at[n], o_recv.at[j], {"pp": p, "tp": r}).start()
    with jax.named_scope("wait_out2"):
        for j in range(per_stage):
            late = at_end & (j >= per_stage - CORES)

            @pl.when(late)
            def _(j=j):
                core = j % CORES

                @pl.when(core == k)
                def _():
                    wait(gbuf.at[core, 0:chips - 1], g_recv.at[core])

                @pl.when(core != k)
                def _():
                    wait(gbuf.at[core], g_recv.at[core])
                for q in range(chips):
                    out_ref[j, :, q * slab:(q + 1) * slab] = _bf16(sum(_f32(gbuf[core, o, q]) for o in range(chips)))

            @pl.when(jnp.logical_not(late))
            def _(j=j):
                @pl.when(j % CORES == k)
                def _():
                    wait(obuf.at[j, 0:chips - 1], o_recv.at[j])

                @pl.when(j % CORES != k)
                def _():
                    wait(obuf.at[j], o_recv.at[j])
                for q in range(chips):
                    out_ref[j, :, q * slab:(q + 1) * slab] = obuf[j, q]

    with jax.named_scope("wait_sends"):
        @pl.when(at_start)
        def _():
            wait(hx.at[0], h_send)
            wait(qrecv, q_send)
        for n in range(per_core):
            @pl.when(jnp.logical_not(at_end & (n == per_core - 1)))
            def _(n=n):
                wait(tbuf.at[n, 0:ranks - 1], o_send.at[n])

        @pl.when(at_end)
        def _():
            wait(fbuf.at[:, 0:ranks - 1], g_send)
        for par in range(2):
            @pl.when(at_end & (par == 0))
            def _(par=par):
                wait(sbuf.at[par, 0:3], rs_send.at[par])

            @pl.when(jnp.logical_not(at_end))
            def _(par=par):
                wait(sbuf.at[par], rs_send.at[par])
            wait(ybuf.at[0, 0:3], ag_send.at[par])
            wait(stat.at[0, 0:3], st_send.at[par])
        for v in range(2):
            @pl.when((v == 1) | jnp.logical_not(at_start))
            def _(v=v):
                for j in range(2):
                    push_w(v, j).wait_send()

        @pl.when(jnp.logical_not(at_start | at_end))
        def _():
            x_load.wait()

        @pl.when(at_start)
        def _():
            wait(xs.at[0:visits], x_send.at[c])
            for chip in (far, right, left):
                wait(xs.at[0:CORES * OWN_SHARE], x_send.at[chip])

        @pl.when(at_end)
        def _():
            for chip in (far, right, left):
                wait(xs.at[0:CORES * (visits - OWN_SHARE)], x_send.at[chip])


def solution(mesh):
    stages, ranks = mesh.shape["pp"], mesh.shape["tp"]
    chips = ranks // CORES

    def per_device(x, gain, w_in, w_out):
        micro, tsh, width = x.shape
        passes, _, _, hid = w_in.shape
        tok = tsh * ranks
        visits = micro // CORES
        half = width // chips // 2
        per_stage = micro // stages
        dims = (stages, chips, visits, tok, width, hid)
        bf = jnp.bfloat16
        dma = pltpu.SemaphoreType.DMA
        any_space = pl.BlockSpec(memory_space=pl.ANY)
        vmem = pl.BlockSpec(memory_space=pltpu.VMEM)
        return pl.pallas_call(
            functools.partial(_kernel, dims),
            name="mlp_pipe",
            out_shape=jax.ShapeDtypeStruct((per_stage, tsh, width), bf),
            in_specs=[any_space, vmem, any_space, any_space],
            out_specs=vmem,
            scratch_shapes=[
                pltpu.VMEM((passes, CORES, width, hid), bf),
                pltpu.VMEM((passes, CORES, hid, width), bf),
                pltpu.VMEM((micro, tsh, width), bf),
                pltpu.VMEM((visits, ranks, tsh, width), bf),
                pltpu.VMEM((visits, chips, 2, tok, half), bf),
                pltpu.VMEM((visits, 3, 2, tok, half), bf),
                pltpu.VMEM((visits, chips, 8, 128), jnp.float32),
                pltpu.VMEM((2, tok, 128), jnp.float32),
                pltpu.VMEM((3, 2, tok, half), bf),
                pltpu.VMEM((2, 2, tok, half), jnp.float32),
                pltpu.VMEM((tok, 2 * half), bf),
                pltpu.VMEM((CORES, tok, hid), jnp.float32),
                pltpu.VMEM((CORES, tok, width), bf),
                pltpu.VMEM((chips, CORES, tok, 2 * half), bf),
                pltpu.VMEM((chips, tok, 2 * half), bf),
                pltpu.VMEM((CORES, tok, hid), bf),
                pltpu.VMEM((2, chips, 2, tok, half), bf),
                pltpu.VMEM((per_stage // CORES, ranks, tsh, 2 * half), bf),
                pltpu.VMEM((per_stage, chips, tsh, 2 * half), bf),
                pltpu.VMEM((chips, ranks, tsh, 2 * half), bf),
                pltpu.VMEM((CORES, chips, chips, tsh, 2 * half), bf),
                dma((passes, 2)), dma((passes, 2)), dma((passes, 2)),
                dma, dma((chips,)), dma((visits,)), pltpu.SemaphoreType.REGULAR,
                dma((2,)), dma((visits,)), dma((3, 2)), dma((2,)), dma((visits, 2)), dma((visits,)), dma((visits,)), dma((2,)), dma((visits,)),
                dma((per_stage // CORES,)), dma((per_stage,)), dma, dma, dma, dma((chips,)), dma, dma((CORES,)),
            ],
            compiler_params=pltpu.CompilerParams(collective_id=0, has_side_effects=True, flags=FLAGS, vmem_limit_bytes=67043328),
        )(x, gain, w_in.reshape(passes, width, hid), w_out.reshape(passes, hid, width))

    return jax.shard_map(
        per_device,
        mesh=mesh,
        in_specs=(P("dp", "tp", None), P(None, "pp", None), P(None, "pp", None, "tp"), P(None, "pp", "tp", None)),
        out_specs=P(("dp", "pp"), "tp", None),
        check_vma=False,
    )
```

```python
import functools

import jax
import jax.numpy as jnp
from jax import lax
from jax.experimental import pallas as pl
from jax.experimental.pallas import tpu as pltpu
from jax.sharding import PartitionSpec as P

MESH = pl.DeviceIdType.MESH
NORM_EPS = 1e-5
CORES = 2
OWN_SHARE = 2
ORDER = (0, 1, 2, 3)
FIRST_ORDER = (3, 0, 1, 2)
REDUCE_AT = 4
LEAD_AT = 5
LEADS = 2
FORWARD_AT = 10
LEAD_FWD = 10
FLAGS = {}
ADD_AT = 4
ADD_LEADS = 2
TILE = 256


def _f32(a):
    return a.astype(jnp.float32)


def _bf16(a):
    return a.astype(jnp.bfloat16)


def _kernel(dims, x_hbm, gain_ref, w1_hbm, w2_hbm, out_ref,
            w1, w2, xs, xbuf, ybuf, rbuf, stat, norm, lbuf, hold, hbuf, accb, hx, qbuf, qrecv, abuf, sbuf, tbuf, obuf, fbuf, gbuf,
            wl_sem, wp_send, wp_recv, xl_sem, x_send, x_recv, ready,
            rs_send, rs_recv, l_recv, ag_send, ag_first, ag_near, ag_far, st_send, st_recv, o_send, o_recv, h_send, h_recv, q_send, q_recv, g_send, g_recv):
    stages, chips, visits, tok, width, hid = dims
    ranks = chips * CORES
    slab = width // chips
    half = slab // 2
    tsh = tok // ranks
    per_stage = visits * CORES // stages
    p = lax.axis_index("pp")
    t = lax.axis_index("tp")
    c = t // CORES
    k = lax.rem(t, CORES)
    nxt = lax.rem(p + 1, stages)
    right, left = lax.rem(c + 1, chips), lax.rem(c + chips - 1, chips)
    far = lax.rem(c + 2, chips)
    at_start = p == 0
    at_end = p == stages - 1

    def dev(pp, chip, core):
        return {"pp": pp, "tp": chip * CORES + core}

    def remote(src, dst, ssem, rsem, where):
        return pltpu.make_async_remote_copy(src_ref=src, dst_ref=dst, send_sem=ssem, recv_sem=rsem,
                                            device_id=where, device_id_type=MESH)

    def wait(ref, sem):
        pltpu.make_async_copy(ref, ref, sem).wait()

    def load_w(v, j):
        src, dst = ((w1_hbm, w1), (w2_hbm, w2))[j]
        return pltpu.make_async_copy(src.at[v], dst.at[v, k], wl_sem.at[v, j])

    def push_w(v, j):
        src, dst = ((w1_hbm, w1), (w2_hbm, w2))[j]
        return remote(src.at[v], dst.at[v, k], wp_send.at[v, j], wp_recv.at[v, j], dev(p, c, 1 - k))

    def push_piece(i):
        for j, (src, dst) in enumerate(((w1_hbm, w1), (w2_hbm, w2))):
            size = src.shape[1] // visits
            rows = pl.ds(pl.multiple_of(i * size, size), size)
            remote(src.at[1, rows], dst.at[1, k, rows], wp_send.at[1, j], wp_recv.at[1, j], dev(p, c, 1 - k)).start()

    x_load = pltpu.make_async_copy(x_hbm, xs, xl_sem)
    x_load.start()
    for v in range(2):
        for j in range(2):
            load_w(v, j).start()

    bar = pltpu.get_barrier_semaphore()
    for r in range(ranks):
        @pl.when(r != t)
        def _(r=r):
            pl.semaphore_signal(bar, inc=1, device_id={"pp": p, "tp": r}, device_id_type=MESH)

    @pl.when(jnp.logical_not(at_end))
    def _():
        for q in range(chips):
            pl.semaphore_signal(bar, inc=1, device_id=dev(nxt, q, k), device_id_type=MESH)

    @pl.when(at_start)
    def _():
        for r in range(ranks):
            pl.semaphore_signal(bar, inc=1, device_id={"pp": stages - 1, "tp": r}, device_id_type=MESH)
    known = jnp.where(at_start, ranks - 1, jnp.where(at_end, 2 * ranks - 1 + chips, ranks - 1 + chips))
    pl.semaphore_wait(bar, known)

    @pl.when(jnp.logical_not(at_start))
    def _():
        for q in range(chips):
            pl.semaphore_signal(ready, inc=1, device_id=dev(p - 1, q, k), device_id_type=MESH)

    def x_copy(i, core, chip):
        return remote(xs.at[CORES * i + core], xbuf.at[i, t], x_send.at[chip], x_recv.at[i], dev(0, chip, core))

    def x_share(i):
        for core in range(CORES):
            for chip in (far, right, left):
                x_copy(i, core, chip).start()

    @pl.when(at_start)
    def _():
        x_load.wait()
        for i in range(visits):
            x_copy(i, 1 - k, c).start()
        for i in range(OWN_SHARE):
            x_share(i)

    @pl.when(at_end)
    def _():
        x_load.wait()
        for i in range(OWN_SHARE, visits):
            x_share(i)

    @pl.when(jnp.logical_not(at_start))
    def _():
        for v in range(2):
            for j in range(2):
                push_w(v, j).start()

    def share(i, par, owner, h, chip, sem):
        return remote(ybuf.at[i, owner, h], ybuf.at[i, owner, h], ag_send.at[par], sem, dev(p, chip, k))

    def reduce_slab(idx):
        i = lax.rem(idx, visits)
        par = lax.rem(idx, 2)

        @pl.when(idx >= jnp.where(at_start, visits + 2, 2))
        def _():
            wait(ybuf.at[i, 0:3], ag_send.at[par])
            wait(stat.at[i, 0:3], st_send.at[par])

        with jax.named_scope("wait_rs"):
            wait(rbuf.at[i], rs_recv.at[i])
        own = [_bf16(_f32(rbuf[i, 0, h]) + _f32(rbuf[i, 1, h]) + _f32(rbuf[i, 2, h])) for h in range(2)]
        for h in range(2):
            ybuf[i, c, h] = own[h]
        share(i, par, c, 0, right, ag_first.at[i, 0]).start()
        share(i, par, c, 1, left, ag_first.at[i, 1]).start()
        own = [_f32(a) for a in own]
        mean = sum(jnp.sum(a, axis=-1, keepdims=True) for a in own) * (1.0 / slab)
        dev2 = sum(jnp.sum((a - mean) * (a - mean), axis=-1, keepdims=True) for a in own)
        lane = lax.broadcasted_iota(jnp.int32, (8, 128), 1)
        tile = jnp.zeros((8, 128), jnp.float32)
        for j, col in enumerate((mean, dev2)):
            for a in range(tok // 8):
                tile = jnp.where(lane == tok // 8 * j + a, col[8 * a:8 * a + 8, :], tile)
        stat[i, c] = tile
        for chip in (far, right, left):
            remote(stat.at[i, c], stat.at[i, c], st_send.at[par], st_recv.at[i], dev(p, chip, k)).start()
        share(i, par, c, 1, right, ag_near.at[i]).start()
        share(i, par, c, 0, left, ag_near.at[i]).start()

    def forward(idx):
        i = lax.rem(idx, visits)
        par = lax.rem(idx, 2)
        with jax.named_scope("wait_fwd"):
            wait(ybuf.at[i, left, 0], ag_first.at[i, 0])
            share(i, par, left, 0, right, ag_far.at[i]).start()
            wait(ybuf.at[i, right, 1], ag_first.at[i, 1])
            share(i, par, right, 1, left, ag_far.at[i]).start()

    @pl.when(jnp.logical_not(at_start))
    def _():
        reduce_slab(0)
        forward(0)

    def add_relayed(idx):
        i = lax.rem(idx, visits)
        par = lax.rem(idx, 2)
        dst = jnp.where(at_end & (idx >= visits), CORES * i // per_stage, nxt)
        for slot, chip, h in ((1, right, 0), (2, left, 1)):
            got = lax.rem(idx, 3)
            with jax.named_scope("wait_l"):
                wait(lbuf.at[got, h], l_recv.at[got, h])
            sbuf[par, slot, h] = _bf16(hold[par, h] + _f32(lbuf[got, h]))
            remote(sbuf.at[par, slot, h], rbuf.at[i, slot, h], rs_send.at[par], rs_recv.at[i], dev(dst, chip, k)).start()

    def visit(kind, idx, carry):
        v = 0 if kind == "first" else idx // visits
        i = lax.rem(idx, visits)
        dst = jnp.where(at_end & (v == 1), CORES * i // per_stage, nxt)
        par = lax.rem(idx, 2)

        def at(place):
            if kind == "last":
                if place == ADD_AT and place < 10:
                    add_relayed(idx - 1)
                return
            if place == ADD_AT and place < 10:
                @pl.when(i > ADD_LEADS)
                def _():
                    add_relayed(idx - 1)
            if kind == "first":
                return
            ahead = (idx + 1 < 2 * visits) & (idx + 1 != visits)
            if place == REDUCE_AT:
                @pl.when(ahead & (i >= LEADS))
                def _():
                    reduce_slab(idx + 1)
            if place == LEAD_AT:
                @pl.when(ahead & (i < LEADS))
                def _():
                    reduce_slab(idx + 1)
            if place == LEAD_FWD and LEAD_FWD < 11:
                @pl.when(ahead & (i < LEADS))
                def _():
                    forward(idx + 1)
            if place == FORWARD_AT:
                @pl.when(ahead & (i >= LEADS))
                def _():
                    forward(idx + 1)

        if kind == "first":
            xbuf[i, t] = xs[CORES * i + k]
            with jax.named_scope("wait_x"):
                wait(xbuf.at[i, 0:ranks - 1], x_recv.at[i])
            for q in range(chips):
                for h in range(2):
                    lo = q * slab + h * half
                    ybuf[i, q, h] = _bf16(_f32(xbuf[i, :, :, lo:lo + half]).reshape(tok, half))

        at(1)

        def keep(mean, scale):
            norm[0] = jnp.broadcast_to(mean, (tok, 128))
            norm[1] = jnp.broadcast_to(scale, (tok, 128))

        if kind == "first":
            pieces = [(q, h) for q in range(chips) for h in range(2)]
            mean = sum(jnp.sum(_f32(ybuf[i, q, h]), axis=-1, keepdims=True) for q, h in pieces) * (1.0 / width)
            var = jnp.zeros_like(mean)
            for q, h in pieces:
                a = _f32(ybuf[i, q, h]) - mean
                var = var + jnp.sum(a * a, axis=-1, keepdims=True)
            keep(mean, lax.rsqrt(var * (1.0 / width) + NORM_EPS))

        else:
            with jax.named_scope("wait_st"):
                wait(stat.at[i, 0:3], st_recv.at[i])
            groups = tok // 8
            means = [stat[i, q][:, :groups] for q in range(chips)]
            devs = [stat[i, q][:, groups:2 * groups] for q in range(chips)]
            mean = sum(means) * (1.0 / chips)
            dev2 = sum(devs[q] + slab * (means[q] - mean) * (means[q] - mean) for q in range(chips))
            scale = lax.rsqrt(dev2 * (1.0 / width) + NORM_EPS)
            for a in range(groups):
                rows = slice(8 * a, 8 * a + 8)
                norm[0, rows] = jnp.broadcast_to(mean[:, a:a + 1], (8, 128))
                norm[1, rows] = jnp.broadcast_to(scale[:, a:a + 1], (8, 128))

        def wait_weights(j):
            @pl.when(i == 0)
            def _():
                load_w(v, j).wait()
                if kind != "first":
                    push_w(v, j).wait_recv()

        with jax.named_scope("wait_w1"):
            wait_weights(0)
        at(2)
        tile = TILE
        if kind == "first":
            @pl.when(i > 0)
            def _():
                wait(hx.at[0], h_send)
            for q in range(chips):
                for m in range(slab // 128):
                    cols = slice(q * slab + m * 128, q * slab + (m + 1) * 128)
                    h, lo = m * 128 // half, m * 128 % half
                    hx[k, :, cols] = _bf16((_f32(ybuf[i, q, h, :, lo:lo + 128]) - norm[0]) * norm[1] * _f32(gain_ref[v, :, cols]))
            remote(hx.at[k], hx.at[k], h_send, h_recv, dev(p, c, 1 - k)).start()

            @pl.when(i > 0)
            def _():
                add_relayed(idx - 1)
            with jax.named_scope("wait_h"):
                wait(hx.at[0], h_recv)
            for col in range(0, hid, 2 * tile):
                cols = slice(col, col + 2 * tile)
                part = jnp.dot(hx[...].reshape(CORES * tok, width), w1[v, k, :, cols], preferred_element_type=jnp.float32)
                abuf[:, :, cols] = _bf16(jax.nn.gelu(part)).reshape(CORES, tok, 2 * tile)
        for n_done, chip in enumerate((c, right, left, far) if kind != "first" else ()):
            if n_done in (1, 3):
                with jax.named_scope("wait_ag"):
                    wait(ybuf.at[i, 0], (None, ag_near, None, ag_far)[n_done].at[i])
            for m in range(slab // 128):
                cols = slice(m * 128, (m + 1) * 128)
                gain = gain_ref[v, :, pl.ds(pl.multiple_of(chip * slab + m * 128, 128), 128)]
                h, lo = m * 128 // half, m * 128 % half
                hbuf[:, cols] = _bf16((_f32(ybuf[i, chip, h, :, lo:lo + 128]) - norm[0]) * norm[1] * _f32(gain))
            for s in range(CORES):
                for col in range(0, hid, 2 * tile):
                    rows = pl.ds(pl.multiple_of(chip * slab, slab), slab)
                    cols = slice(col, col + 2 * tile)
                    part = jnp.dot(hbuf[...], w1[v, s, rows, cols], preferred_element_type=jnp.float32)
                    if n_done:
                        part = part + accb[s, :, cols]
                    if n_done < 3:
                        accb[s, :, cols] = part
                    else:
                        abuf[s, :, cols] = _bf16(jax.nn.gelu(part))
            if n_done < 3:
                at(3 + n_done)
        at(6)
        with jax.named_scope("wait_w2"):
            wait_weights(1)

        @pl.when(idx == 0)
        def _():
            @pl.when(jnp.logical_not(at_end))
            def _():
                pl.semaphore_wait(ready, chips)

        @pl.when(idx >= 2)
        def _():
            wait(sbuf.at[par], rs_send.at[par])

        def partial(slot, h, dst, where, sem):
            return remote(sbuf.at[par, slot, h], dst, rs_send.at[par], sem, where)

        row_chip = lax.broadcasted_iota(jnp.int32, (tok, slab), 0) // (tsh * CORES)

        def tokens_done(n, q, prod):
            whole = jnp.concatenate([_f32(ybuf[i, q, 0]), _f32(ybuf[i, q, 1])], axis=1)
            fbuf[n] = _bf16((prod + jnp.where(row_chip == c, whole, 0.0)).reshape(ranks, tsh, slab))
            for r in range(ranks):
                @pl.when(r == t)
                def _(r=r):
                    gbuf[k, c, q] = fbuf[n, r]

                @pl.when(r != t)
                def _(r=r):
                    remote(fbuf.at[n, r], gbuf.at[k, c, q], g_send, g_recv.at[k], {"pp": p, "tp": r}).start()

        def slab_done(n, q, prod):
            if kind == "last":
                return tokens_done(n, q, prod)
            prod = prod[:, :half], prod[:, half:]
            if n == 0:
                got = lax.rem(idx, 3)
                for h, chip in ((0, right), (1, left)):
                    sbuf[par, 0, h] = _bf16(prod[h])
                    partial(0, h, lbuf.at[got, h], dev(p, chip, k), l_recv.at[got, h]).start()
            elif n == 3:
                for h in range(2):
                    sbuf[par, 3, h] = _bf16(prod[h] + _f32(ybuf[i, c, h]))


                @pl.when(dst != p)
                def _():
                    remote(sbuf.at[par, 3], rbuf.at[i, 0], rs_send.at[par], rs_recv.at[i], dev(dst, c, k)).start()

                @pl.when(dst == p)
                def _():
                    rbuf[i, 0] = sbuf[par, 3]
            else:
                h = 2 - n
                sbuf[par, n, h] = _bf16(prod[h])
                hold[par, 1 - h] = prod[1 - h]
                partial(n, h, rbuf.at[i, n, h], dev(dst, q, k), rs_recv.at[i]).start()

        order = (far, right, left, c)
        if kind == "first":
            @pl.when(i > 0)
            def _():
                wait(qrecv, q_send)
            for n in FIRST_ORDER:
                q = order[n]
                cols = pl.ds(pl.multiple_of(q * slab, slab), slab)
                prod = jnp.dot(abuf[...].reshape(CORES * tok, hid), w2[v, k, :, cols], preferred_element_type=jnp.float32)
                qbuf[n] = _bf16(prod).reshape(CORES, tok, slab)
                remote(qbuf.at[n, 1 - k], qrecv.at[n], q_send, q_recv.at[n], dev(p, c, 1 - k)).start()
            for n in FIRST_ORDER:
                q = order[n]
                with jax.named_scope("wait_q"):
                    wait(qrecv.at[n], q_recv.at[n])
                slab_done(n, q, _f32(qbuf[n, k]) + _f32(qrecv[n]))
            push_piece(i)
        for m, n in enumerate(ORDER if kind != "first" else ()):
            q = order[n]
            cols = pl.ds(pl.multiple_of(q * slab, slab), slab)
            prod = jnp.zeros((tok, slab), jnp.float32)
            for s in range(CORES):
                prod = prod + _f32(_bf16(jnp.dot(abuf[s], w2[v, s, :, cols], preferred_element_type=jnp.float32)))
            slab_done(n, q, prod)
            if m < 3:
                at(7 + m)
        at(10)
        if kind == "last":
            return carry

        @pl.when((i == visits - 1) if kind == "first" else (i < ADD_LEADS) | (i == visits - 1) | (ADD_AT > 9))
        def _():
            add_relayed(idx)
        at(11)
        if kind == "mid":
            @pl.when((LEAD_FWD > 10) & (i < LEADS) & (idx + 1 < 2 * visits) & (idx + 1 != visits))
            def _():
                forward(idx + 1)

        @pl.when(idx + 1 == visits)
        def _():
            reduce_slab(idx + 1)
            forward(idx + 1)

        return carry

    mid_from = jnp.where(at_start, visits, 0)
    lax.fori_loop(0, mid_from, functools.partial(visit, "first"), 0)
    lax.fori_loop(mid_from, 2 * visits - jnp.where(at_end, 1, 0), functools.partial(visit, "mid"), 0)

    @pl.when(at_end)
    def _():
        visit("last", 2 * visits - 1, 0)

    per_core = per_stage // CORES
    with jax.named_scope("wait_out"):
        for n in range(per_core):
            i = per_core * p + n
            j = CORES * n + k

            @pl.when(jnp.logical_not(at_end & (n == per_core - 1)))
            def _(n=n, i=i, j=j):
                @pl.when(at_end)
                def _(i=i):
                    wait(rbuf.at[i, 0:2], rs_recv.at[i])

                @pl.when(jnp.logical_not(at_end))
                def _(i=i):
                    wait(rbuf.at[i], rs_recv.at[i])
                for h in range(2):
                    total = _bf16(_f32(rbuf[i, 0, h]) + _f32(rbuf[i, 1, h]) + _f32(rbuf[i, 2, h]))
                    tbuf[n, :, :, h * half:(h + 1) * half] = _bf16(_f32(total).reshape(ranks, tsh, half))
                for r in range(ranks):
                    @pl.when(r == t)
                    def _(r=r, n=n, j=j):
                        obuf[j, c] = tbuf[n, r]

                    @pl.when(r != t)
                    def _(r=r, n=n, j=j):
                        remote(tbuf.at[n, r], obuf.at[j, c], o_send.at[n], o_recv.at[j], {"pp": p, "tp": r}).start()
    with jax.named_scope("wait_out2"):
        for j in range(per_stage):
            late = at_end & (j >= per_stage - CORES)

            @pl.when(late)
            def _(j=j):
                core = j % CORES

                @pl.when(core == k)
                def _():
                    wait(gbuf.at[core, 0:chips - 1], g_recv.at[core])

                @pl.when(core != k)
                def _():
                    wait(gbuf.at[core], g_recv.at[core])
                for q in range(chips):
                    out_ref[j, :, q * slab:(q + 1) * slab] = _bf16(sum(_f32(gbuf[core, o, q]) for o in range(chips)))

            @pl.when(jnp.logical_not(late))
            def _(j=j):
                @pl.when(j % CORES == k)
                def _():
                    wait(obuf.at[j, 0:chips - 1], o_recv.at[j])

                @pl.when(j % CORES != k)
                def _():
                    wait(obuf.at[j], o_recv.at[j])
                for q in range(chips):
                    out_ref[j, :, q * slab:(q + 1) * slab] = obuf[j, q]

    with jax.named_scope("wait_sends"):
        @pl.when(at_start)
        def _():
            wait(hx.at[0], h_send)
            wait(qrecv, q_send)
        for n in range(per_core):
            @pl.when(jnp.logical_not(at_end & (n == per_core - 1)))
            def _(n=n):
                wait(tbuf.at[n, 0:ranks - 1], o_send.at[n])

        @pl.when(at_end)
        def _():
            wait(fbuf.at[:, 0:ranks - 1], g_send)
        for par in range(2):
            @pl.when(at_end & (par == 0))
            def _(par=par):
                wait(sbuf.at[par, 0:3], rs_send.at[par])

            @pl.when(jnp.logical_not(at_end))
            def _(par=par):
                wait(sbuf.at[par], rs_send.at[par])
            wait(ybuf.at[0, 0:3], ag_send.at[par])
            wait(stat.at[0, 0:3], st_send.at[par])
        for v in range(2):
            @pl.when((v == 1) | jnp.logical_not(at_start))
            def _(v=v):
                for j in range(2):
                    push_w(v, j).wait_send()

        @pl.when(jnp.logical_not(at_start | at_end))
        def _():
            x_load.wait()

        @pl.when(at_start)
        def _():
            wait(xs.at[0:visits], x_send.at[c])
            for chip in (far, right, left):
                wait(xs.at[0:CORES * OWN_SHARE], x_send.at[chip])

        @pl.when(at_end)
        def _():
            for chip in (far, right, left):
                wait(xs.at[0:CORES * (visits - OWN_SHARE)], x_send.at[chip])


def solution(mesh):
    stages, ranks = mesh.shape["pp"], mesh.shape["tp"]
    chips = ranks // CORES

    def per_device(x, gain, w_in, w_out):
        micro, tsh, width = x.shape
        passes, _, _, hid = w_in.shape
        tok = tsh * ranks
        visits = micro // CORES
        half = width // chips // 2
        per_stage = micro // stages
        dims = (stages, chips, visits, tok, width, hid)
        bf = jnp.bfloat16
        dma = pltpu.SemaphoreType.DMA
        any_space = pl.BlockSpec(memory_space=pl.ANY)
        vmem = pl.BlockSpec(memory_space=pltpu.VMEM)
        return pl.pallas_call(
            functools.partial(_kernel, dims),
            name="mlp_pipe",
            out_shape=jax.ShapeDtypeStruct((per_stage, tsh, width), bf),
            in_specs=[any_space, vmem, any_space, any_space],
            out_specs=vmem,
            scratch_shapes=[
                pltpu.VMEM((passes, CORES, width, hid), bf),
                pltpu.VMEM((passes, CORES, hid, width), bf),
                pltpu.VMEM((micro, tsh, width), bf),
                pltpu.VMEM((visits, ranks, tsh, width), bf),
                pltpu.VMEM((visits, chips, 2, tok, half), bf),
                pltpu.VMEM((visits, 3, 2, tok, half), bf),
                pltpu.VMEM((visits, chips, 8, 128), jnp.float32),
                pltpu.VMEM((2, tok, 128), jnp.float32),
                pltpu.VMEM((3, 2, tok, half), bf),
                pltpu.VMEM((2, 2, tok, half), jnp.float32),
                pltpu.VMEM((tok, 2 * half), bf),
                pltpu.VMEM((CORES, tok, hid), jnp.float32),
                pltpu.VMEM((CORES, tok, width), bf),
                pltpu.VMEM((chips, CORES, tok, 2 * half), bf),
                pltpu.VMEM((chips, tok, 2 * half), bf),
                pltpu.VMEM((CORES, tok, hid), bf),
                pltpu.VMEM((2, chips, 2, tok, half), bf),
                pltpu.VMEM((per_stage // CORES, ranks, tsh, 2 * half), bf),
                pltpu.VMEM((per_stage, chips, tsh, 2 * half), bf),
                pltpu.VMEM((chips, ranks, tsh, 2 * half), bf),
                pltpu.VMEM((CORES, chips, chips, tsh, 2 * half), bf),
                dma((passes, 2)), dma((passes, 2)), dma((passes, 2)),
                dma, dma((chips,)), dma((visits,)), pltpu.SemaphoreType.REGULAR,
                dma((2,)), dma((visits,)), dma((3, 2)), dma((2,)), dma((visits, 2)), dma((visits,)), dma((visits,)), dma((2,)), dma((visits,)),
                dma((per_stage // CORES,)), dma((per_stage,)), dma, dma, dma, dma((chips,)), dma, dma((CORES,)),
            ],
            compiler_params=pltpu.CompilerParams(collective_id=0, has_side_effects=True, flags=FLAGS, vmem_limit_bytes=67043328),
        )(x, gain, w_in.reshape(passes, width, hid), w_out.reshape(passes, hid, width))

    return jax.shard_map(
        per_device,
        mesh=mesh,
        in_specs=(P("dp", "tp", None), P(None, "pp", None), P(None, "pp", None, "tp"), P(None, "pp", "tp", None)),
        out_specs=P(("dp", "pp"), "tp", None),
        check_vma=False,
    )
```
